256 devices in a mesh: row: 32 (over x, z), col: 8 (over y, core).
Axes of the slice: x: 4, y: 4, z: 8, core: 2. Of those that a mesh axis runs over, the one named last changes fastest.
Arguments:
- diag_tiles: float32 [32, 512, 512], P('row', 'col'), as said below
- sub_tiles: float32 [32, 512, 512], P('row', 'col')
- boundary: float32 [512, 512], P('col'), as said below
Outputs:
- inverse_blocks: float32 [32, 512, 512], P('row', 'col')
Inputs may be any that keep to these rules, and one draw needn't show every extreme that they name: `diag_tiles`: every tile is lower triangular, zero above the diagonal, with diagonal entries between 0.2 and 0.4. `boundary`: symmetric positive definite, smallest eigenvalue at least 2.
All inputs are finite; a program needn't handle non-finite values.
Results may differ from the reference program's by a relative error of at most 0.0003.
Values sent between devices are 32-bit elements; how exact they have to be, the bound alone decides.
A program may use at most 256 MiB of HBM per device.

```python
import math
import jax
import jax.numpy as jnp
from jax import lax

B = 512
NBLK = 32


def draw_diag_tiles(key, part):
    first_key = jax.random.fold_in(key, 11)
    second_key = jax.random.fold_in(key, 12)
    diagonal = jnp.exp(jax.random.uniform(first_key, (NBLK, B), jnp.float32, math.log(0.2), math.log(0.4)))
    below = jax.random.normal(second_key, (NBLK, B, B), jnp.float32) * (0.1 / math.sqrt(B))
    strict_mask = jnp.tril(jnp.ones((B, B), jnp.float32), -1)
    identity = jnp.eye(B, dtype=jnp.float32)
    return below * strict_mask + diagonal[:, :, None] * identity


def invert_lower(tile):
    return jax.scipy.linalg.solve_triangular(tile, jnp.eye(B, dtype=jnp.float32), lower=True)


def draw_sub_tiles(key, part):
    inverse_tiles = draw_diag_tiles(key, part)
    lower = jax.vmap(invert_lower)(inverse_tiles)
    orth_key = jax.random.fold_in(key, 21)
    rate_key = jax.random.fold_in(key, 22)
    gauss = jax.random.normal(orth_key, (NBLK, B, B), jnp.float32)
    orthogonal, triangle = jnp.linalg.qr(gauss)
    rates = jax.random.uniform(rate_key, (NBLK,), jnp.float32, 0.5, 1.5)
    gains = jnp.exp(-rates / NBLK)
    coupled = jnp.einsum('kij,kjl->kil', orthogonal, lower, precision=lax.Precision.HIGHEST)
    return gains[:, None, None] * coupled


def draw_boundary(key, part):
    inner_key = jax.random.fold_in(key, 31)
    scale_key = jax.random.fold_in(key, 32)
    factor = jax.random.normal(inner_key, (B, B), jnp.float32)
    level = jnp.exp(jax.random.uniform(scale_key, (), jnp.float32, math.log(2.0), math.log(6.0)))
    gram = jnp.dot(factor, factor.T, precision=lax.Precision.HIGHEST) / B
    return level * (gram + jnp.eye(B, dtype=jnp.float32))


def setup_inputs(seed: int = 0) -> dict:
    key_list = jax.random.split(jax.random.key(seed), 4)
    return {
        "diag_tiles": draw_diag_tiles(jax.random.fold_in(key_list[3], 71), 0),
        "sub_tiles": draw_sub_tiles(jax.random.fold_in(key_list[3], 71), 0),
        "boundary": draw_boundary(jax.random.fold_in(key_list[3], 71), 0),
    }


def product(left, right):
    return jnp.dot(left, right, precision=lax.Precision.HIGHEST)

def reference(diag_tiles, sub_tiles, boundary):

    def step(z_next, tiles):
        tile_inverse, coupling = tiles
        local_term = product(tile_inverse.T, tile_inverse)
        weight = product(coupling, tile_inverse)
        z_here = local_term + product(weight.T, product(z_next, weight))
        return (z_here, z_here)
    final_block, inverse_blocks = lax.scan(step, boundary, (diag_tiles, sub_tiles), reverse=True)
    return inverse_blocks
```

```python
import functools

import jax
import jax.numpy as jnp
from jax import lax
from jax.experimental import pallas as pl
from jax.experimental.pallas import tpu as pltpu

MESH = pl.DeviceIdType.MESH
BF16 = jnp.bfloat16
F32 = jnp.float32


def split(value):
    high = value.astype(BF16)
    low = (value - high.astype(F32)).astype(BF16)
    return high, low


def dot(left, right):
    return jnp.dot(left, right, preferred_element_type=F32)


def product3(left_high, left_low, right_high, right_low):
    rows = left_high.shape[0]
    both = dot(jnp.concatenate([left_high, left_low], axis=0), right_high)
    return both[:rows] + both[rows:] + dot(left_high, right_low)


def kernel(
    rows_total, levels, d_ref, s_ref, b_ref, o_ref,
    full, entry, sums, ends, landed, m_high, m_low, t_high, t_low,
    full_sem, entry_sem, misc_sem, send_sem,
):
    size = d_ref.shape[-1]
    piece = size // 8
    block = size // 4
    row = lax.axis_index("row")
    col = lax.axis_index("col")
    ring = col // 2
    core = col % 2
    right = (ring + 1) % 4
    left = (ring + 3) % 4
    across = (ring + 2) % 4
    partner = (row, 2 * ring + (1 - core))

    def at_ring(place):
        return (row, 2 * place + core)

    def piece_rows(number):
        return pl.ds(pl.multiple_of(number * piece, piece), piece)

    def part(array, number):
        return full.at[array, piece_rows(number)]

    def copy(src, dst, send, recv, device):
        return pltpu.make_async_remote_copy(
            src_ref=src, dst_ref=dst, send_sem=send, recv_sem=recv,
            device_id=device, device_id_type=MESH,
        )

    some = full.at[0, pl.ds(0, piece)]

    def wait_sent(stage, *numbers):
        for number in numbers:
            copy(some, some, send_sem.at[stage, number], misc_sem.at[0], partner).wait_send()

    def wait_part(array, number):
        here = part(array, number)
        copy(here, here, send_sem.at[0, 0], full_sem.at[array, number], partner).wait_recv()

    def wait_entry(stage, half):
        here = entry.at[stage, pl.ds(half * piece, piece)]
        copy(here, here, send_sem.at[0, 0], entry_sem.at[stage, half], partner).wait_recv()

    def send_part(array, number, device, stage, sem):
        here = part(array, number)
        copy(here, here, send_sem.at[stage, sem], full_sem.at[array, number], device).start()

    barrier = pltpu.get_barrier_semaphore()
    greeted = [partner, at_ring(right), at_ring(left)]
    for level in range(levels):
        step = 2**level
        greeted.append(((row + step) % rows_total, col))
        greeted.append(((row + rows_total - step) % rows_total, col))
    for device in greeted:
        pl.semaphore_signal(barrier, inc=1, device_id=device, device_id_type=MESH)
    pl.semaphore_wait(barrier, len(greeted))

    begin = levels + 2
    mine = 2 * ring + core
    forth = (ring + 1 + 2 * core) % 4
    back = (ring + 3 + 2 * core) % 4
    for sem, device in enumerate((at_ring(forth), at_ring(back), partner)):
        copy(d_ref.at[0], part(0, mine), send_sem.at[begin, sem], full_sem.at[0, mine], device).start()

    @pl.when(core == 1)
    def _():
        copy(
            s_ref.at[0], entry.at[0, pl.ds(piece, piece)],
            send_sem.at[begin, 7], entry_sem.at[0, 1], partner,
        ).start()

    own_ends = ends.at[piece_rows(core)]
    copy(b_ref, own_ends, send_sem.at[begin, 8], misc_sem.at[1], partner).start()
    full[0, piece_rows(mine)] = d_ref[0]
    ends[piece_rows(core)] = b_ref[...]
    wait_part(0, 2 * back + core)
    send_part(0, 2 * back + core, at_ring(forth), begin, 3)
    send_part(0, 2 * back + core, partner, begin, 4)
    wait_part(0, 2 * forth + core)
    send_part(0, 2 * forth + core, partner, begin, 5)
    wait_part(0, 2 * across + core)
    send_part(0, 2 * across + core, partner, begin, 6)
    for place in (ring, back, forth, across):
        wait_part(0, 2 * place + (1 - core))
    other_ends = ends.at[piece_rows(1 - core)]
    copy(other_ends, other_ends, send_sem.at[0, 0], misc_sem.at[1], partner).wait_recv()

    def split_full(array):
        for number in range(4):
            rows = pl.ds(number * block, block)
            m_high[rows], m_low[rows] = split(full[array, rows])

    def split_turned(array):
        columns = pl.ds(pl.multiple_of(ring * block, block), block)
        t_high[...], t_low[...] = split(full[array, :, columns].T)

    def times_full(value):
        high, low = split(value)
        return product3(high, low, m_high[...], m_low[...])

    def spread(array, half, stage):
        number = 2 * ring + half
        send_part(array, number, at_ring(right), stage, 2 * half)
        send_part(array, number, at_ring(left), stage, 2 * half + 1)

    @pl.when(core == 0)
    def _():
        def stage_of_maps(stage, source):
            array = stage + 1
            split_full(min(stage, levels + 1))
            step = 2**stage
            for half in range(2):
                value = times_full(source(half))
                number = 2 * ring + half
                full[array, piece_rows(number)] = value
                spread(array, half, stage)
                if stage < levels:
                    @pl.when(row >= step)
                    def _():
                        copy(
                            part(array, number), entry.at[stage + 1, pl.ds(half * piece, piece)],
                            send_sem.at[stage, 14 + half], entry_sem.at[stage + 1, half],
                            (row - step, col),
                        ).start()
                send_part(array, number, partner, stage, 6 + half)
            wait_part(array, 2 * left)
            send_part(array, 2 * left, at_ring(right), stage, 4)
            send_part(array, 2 * left, partner, stage, 8)
            wait_part(array, 2 * right + 1)
            send_part(array, 2 * right + 1, at_ring(left), stage, 5)
            send_part(array, 2 * right + 1, partner, stage, 9)
            for sem, number in enumerate(
                (2 * left + 1, 2 * right, 2 * across, 2 * across + 1), start=10
            ):
                wait_part(array, number)
                send_part(array, number, partner, stage, sem)

        def sent(stage):
            wait_sent(stage, *range(14))
            if stage < levels:
                @pl.when(row >= 2**stage)
                def _():
                    wait_sent(stage, 14, 15)

        def first(half):
            if half == 0:
                return s_ref[0]
            wait_entry(0, 1)
            return entry[0, pl.ds(piece, piece)]

        stage_of_maps(0, first)
        for stage in range(1, levels + 1):
            @pl.when(row + 2**stage <= rows_total)
            def _(stage=stage):
                def arrived(half):
                    wait_entry(stage, half)
                    return entry[stage, pl.ds(half * piece, piece)]

                stage_of_maps(stage, arrived)

        @pl.when(row == 0)
        def _():
            stage_of_maps(levels + 1, lambda half: ends[pl.ds(half * piece, piece)])

        sent(0)
        for stage in range(1, levels + 1):
            @pl.when(row + 2**stage <= rows_total)
            def _(stage=stage):
                sent(stage)

        @pl.when(row == 0)
        def _():
            sent(levels + 1)

        wait_sent(begin, *range(7), 8)
        copy(landed, landed, send_sem.at[0, 0], misc_sem.at[2], partner).wait_recv()
        o_ref[0] = landed[...]

    @pl.when(core == 1)
    def _():
        first_array = levels + 2

        def pass_on(stage, half):
            step = 2**stage

            @pl.when(row >= step)
            def _():
                copy(
                    sums.at[stage, pl.ds(half * piece, piece)],
                    entry.at[stage + 1, pl.ds(half * piece, piece)],
                    send_sem.at[stage, 14 + half], entry_sem.at[stage + 1, half],
                    (row - step, col),
                ).start()

        split_full(0)
        split_turned(0)
        sums[0] = product3(t_high[...], t_low[...], m_high[...], m_low[...])
        pass_on(0, 0)
        pass_on(0, 1)

        for stage in range(1, levels + 1):
            step = 2 ** (stage - 1)
            array = first_array + stage

            @pl.when(row + step <= rows_total)
            def _(stage=stage, step=step, array=array):
                for number in range(8):
                    wait_part(stage, number)
                split_full(stage)
                split_turned(stage)

                @pl.when(row + step == rows_total)
                def _():
                    entry[stage] = ends[...]

                for half in range(2):
                    @pl.when(row + step < rows_total)
                    def _():
                        wait_entry(stage, half)

                    full[array, piece_rows(2 * ring + half)] = times_full(
                        entry[stage, pl.ds(half * piece, piece)]
                    )
                    spread(array, half, stage)

                def term(place):
                    rows = pl.ds(pl.multiple_of(place * block, block), block)
                    high, low = split(full[array, rows])
                    return product3(t_high[:, rows], t_low[:, rows], high, low)

                total = sums[stage - 1] + term(ring)
                wait_part(array, 2 * left)
                send_part(array, 2 * left, at_ring(right), stage, 4)
                wait_part(array, 2 * right + 1)
                send_part(array, 2 * right + 1, at_ring(left), stage, 5)
                wait_part(array, 2 * left + 1)
                total = total + term(left)
                wait_part(array, 2 * right)
                total = total + term(right)
                wait_part(array, 2 * across)
                wait_part(array, 2 * across + 1)
                sums[stage] = total + term(across)

            @pl.when(row + step > rows_total)
            def _(stage=stage):
                sums[stage] = sums[stage - 1]

            if stage < levels:
                pass_on(stage, 0)
                pass_on(stage, 1)

        @pl.when(row == 0)
        def _():
            for number in range(8):
                wait_part(levels + 1, number)
            split_turned(levels + 1)
            for number in range(8):
                wait_part(levels + 2, number)
            split_full(levels + 2)
            sums[levels] = sums[levels] + product3(
                t_high[...], t_low[...], m_high[...], m_low[...]
            )

        copy(
            sums.at[levels, pl.ds(0, piece)], landed,
            send_sem.at[levels + 1, 0], misc_sem.at[2], partner,
        ).start()
        o_ref[0] = sums[levels, pl.ds(piece, piece)]

        for stage in range(levels):
            @pl.when(row >= 2**stage)
            def _(stage=stage):
                wait_sent(stage, 14, 15)

        for stage in range(1, levels + 1):
            @pl.when(row + 2 ** (stage - 1) <= rows_total)
            def _(stage=stage):
                wait_sent(stage, *range(6))

        wait_sent(begin, *range(9))
        wait_sent(levels + 1, 0)


def on_device(rows_total, diag_tiles, sub_tiles, boundary):
    size = diag_tiles.shape[-1]
    levels = rows_total.bit_length() - 1
    piece = size // 8
    block = size // 4
    return pl.pallas_call(
        functools.partial(kernel, rows_total, levels),
        out_shape=jax.ShapeDtypeStruct(diag_tiles.shape, F32),
        in_specs=[pl.BlockSpec(memory_space=pltpu.VMEM)] * 3,
        out_specs=pl.BlockSpec(memory_space=pltpu.VMEM),
        scratch_shapes=[
            pltpu.VMEM((2 * levels + 3, size, size), F32),
            pltpu.VMEM((levels + 1, block, size), F32),
            pltpu.VMEM((levels + 1, block, size), F32),
            pltpu.VMEM((block, size), F32),
            pltpu.VMEM((piece, size), F32),
            pltpu.VMEM((size, size), BF16),
            pltpu.VMEM((size, size), BF16),
            pltpu.VMEM((block, size), BF16),
            pltpu.VMEM((block, size), BF16),
            pltpu.SemaphoreType.DMA((2 * levels + 3, 8)),
            pltpu.SemaphoreType.DMA((levels + 1, 2)),
            pltpu.SemaphoreType.DMA((3,)),
            pltpu.SemaphoreType.DMA((levels + 3, 16)),
        ],
        compiler_params=pltpu.CompilerParams(
            collective_id=0, has_side_effects=True, vmem_limit_bytes=48 * 1024 * 1024
        ),
    )(diag_tiles, sub_tiles, boundary)


def solution(mesh):
    spec = jax.sharding.PartitionSpec
    tiles = spec("row", "col", None)
    return jax.shard_map(
        functools.partial(on_device, mesh.shape["row"]),
        mesh=mesh,
        in_specs=(tiles, tiles, spec("col", None)),
        out_specs=tiles,
        check_vma=False,
    )
```

```python
import functools

import jax
import jax.numpy as jnp
from jax import lax
from jax.experimental import pallas as pl
from jax.experimental.pallas import tpu as pltpu

MESH = pl.DeviceIdType.MESH
BF16 = jnp.bfloat16
F32 = jnp.float32


def split(value):
    high = value.astype(BF16)
    low = (value - high.astype(F32)).astype(BF16)
    return high, low


def dot(left, right):
    return jnp.dot(left, right, preferred_element_type=F32)


def product3(left_high, left_low, right_high, right_low):
    rows = left_high.shape[0]
    both = dot(jnp.concatenate([left_high, left_low], axis=0), right_high)
    return both[:rows] + both[rows:] + dot(left_high, right_low)


def kernel(
    rows_total, levels, d_ref, s_ref, b_ref, o_ref,
    full, sums, landed, m_high, m_low, t_high, t_low,
    full_sem, misc_sem, send_sem,
):
    maps_end = levels
    s_array = 2 * levels + 1
    b_array = 2 * levels + 2
    size = d_ref.shape[-1]
    chunk = size // 8
    block = size // 4
    piece = size // 16
    row = lax.axis_index("row")
    col = lax.axis_index("col")
    ring = col // 2
    core = col % 2
    right = (ring + 1) % 4
    left = (ring + 3) % 4
    across = (ring + 2) % 4
    partner = (row, 2 * ring + (1 - core))
    to_right = (row, 2 * right + core)
    to_left = (row, 2 * left + core)
    last = rows_total - 1

    def rows_of(number, length):
        return pl.ds(pl.multiple_of(number * length, length), length)

    def part(array, number):
        return full.at[array, rows_of(number, piece)]

    def copy(src, dst, send, recv, device):
        return pltpu.make_async_remote_copy(
            src_ref=src, dst_ref=dst, send_sem=send, recv_sem=recv,
            device_id=device, device_id_type=MESH,
        )

    some = full.at[0, pl.ds(0, piece)]

    def wait_sent(stage, numbers):
        for number in numbers:
            copy(some, some, send_sem.at[stage, number], misc_sem.at[0], partner).wait_send()

    def wait_part(array, number):
        here = part(array, number)
        copy(here, here, send_sem.at[0, 0], full_sem.at[array, number], partner).wait_recv()

    def send_part(array, number, device, stage, sem):
        here = part(array, number)
        copy(here, here, send_sem.at[stage, sem], full_sem.at[array, number], device).start()

    mine = 2 * ring + core
    own_rows = rows_of(mine, chunk)
    fetches = [
        pltpu.make_async_copy(ref, full.at[array, own_rows], misc_sem.at[1 + k])
        for k, (ref, array) in enumerate(
            ((d_ref.at[0], 0), (s_ref.at[0], s_array), (b_ref, b_array))
        )
    ]
    for fetch in fetches:
        fetch.start()

    barrier = pltpu.get_barrier_semaphore()
    greeted = [partner, to_right, to_left]
    for level in range(levels):
        step = 2**level
        greeted.append(((row + step) % rows_total, col))
        greeted.append(((row + rows_total - step) % rows_total, col))
    for device in greeted:
        pl.semaphore_signal(barrier, inc=1, device_id=device, device_id_type=MESH)
    for fetch in fetches:
        fetch.wait()
    pl.semaphore_wait(barrier, len(greeted))

    def number_of(place, half):
        return 4 * place + 2 * core + half

    def gather_own(array, stage):
        for half in range(2):
            send_part(array, number_of(ring, half), to_right, stage, half)
            send_part(array, number_of(ring, 1 - half), to_left, stage, 2 + half)
        for half in range(2):
            send_part(array, number_of(ring, half), partner, stage, 4 + half)

    def gather_near(array, stage):
        wait_part(array, number_of(left, 0))
        send_part(array, number_of(left, 0), to_right, stage, 6)
        wait_part(array, number_of(right, 1))
        send_part(array, number_of(right, 1), to_left, stage, 7)
        send_part(array, number_of(left, 0), partner, stage, 8)
        send_part(array, number_of(right, 1), partner, stage, 9)
        wait_part(array, number_of(left, 1))
        send_part(array, number_of(left, 1), partner, stage, 10)
        wait_part(array, number_of(right, 0))
        send_part(array, number_of(right, 0), partner, stage, 11)

    def gather_far(array, stage):
        for half in range(2):
            wait_part(array, number_of(across, half))
            send_part(array, number_of(across, half), partner, stage, 12 + half)

    def gather_partner(array):
        for place in (ring, left, right, across):
            for half in range(2):
                wait_part(array, 4 * place + 2 * (1 - core) + half)

    at_d, at_s, at_b = levels + 1, levels + 2, levels + 3
    gather_own(0, at_d)
    gather_near(0, at_d)
    gather_own(s_array, at_s)
    gather_far(0, at_d)
    gather_near(s_array, at_s)

    @pl.when(row == last)
    def _():
        gather_own(b_array, at_b)

    gather_partner(0)

    def split_full(array):
        for place in range(4):
            rows = pl.ds(place * block, block)
            m_high[rows], m_low[rows] = split(full[array, rows])

    def split_turned(array):
        columns = rows_of(ring, block)
        t_high[...], t_low[...] = split(full[array, :, columns].T)

    def times_full(value):
        high, low = split(value)
        return product3(high, low, m_high[...], m_low[...])

    def weight_rows(place):
        rows = rows_of(place, block)
        full[1, rows] = times_full(full[s_array, rows])

    def rest_of_weight():
        gather_far(s_array, at_s)
        gather_partner(s_array)

        @pl.when(row == last)
        def _():
            gather_near(b_array, at_b)
            gather_far(b_array, at_b)
            gather_partner(b_array)

    split_full(0)

    @pl.when(core == 0)
    def _():
        def pass_map(stage):
            @pl.when(row >= 2**stage)
            def _():
                for quarter in range(4):
                    number = 4 * ring + quarter
                    copy(
                        part(stage + 1, number), part(maps_end + stage + 1, number),
                        send_sem.at[stage, quarter], full_sem.at[maps_end + stage + 1, number],
                        (row - 2**stage, col),
                    ).start()

        @pl.when(row < last)
        def _():
            for half in range(2):
                wait_part(s_array, 4 * ring + 2 + half)
            weight_rows(ring)
            pass_map(0)

        gather_far(s_array, at_s)
        for place in (left, right, across):
            for half in range(2):
                wait_part(s_array, 4 * place + 2 + half)

        @pl.when(row == last)
        def _():
            for half in range(2):
                wait_part(s_array, 4 * ring + 2 + half)
            gather_near(b_array, at_b)
            gather_far(b_array, at_b)
            gather_partner(b_array)

        @pl.when(row < last)
        def _():
            for place in (left, right, across):
                weight_rows(place)

        for stage in range(1, levels):
            @pl.when(row + 2**stage < rows_total)
            def _(stage=stage):
                array = stage + 1
                split_full(stage)
                for quarter in range(4):
                    wait_part(maps_end + stage, 4 * ring + quarter)
                rows = rows_of(ring, block)
                full[array, rows] = times_full(full[maps_end + stage, rows])
                for slot, (one, other) in enumerate(((0, 1), (2, 3), (1, 0), (3, 2))):
                    send_part(array, 4 * ring + one, to_right, stage, 4 + slot)
                    send_part(array, 4 * ring + other, to_left, stage, 8 + slot)
                if stage < levels - 1:
                    pass_map(stage)
                for quarter in range(4):
                    send_part(array, 4 * ring + quarter, partner, stage, 12 + quarter)
                for slot, quarter in enumerate((0, 2)):
                    wait_part(array, 4 * left + quarter)
                    send_part(array, 4 * left + quarter, to_right, stage, 16 + slot)
                    wait_part(array, 4 * right + quarter + 1)
                    send_part(array, 4 * right + quarter + 1, to_left, stage, 18 + slot)
                    send_part(array, 4 * left + quarter, partner, stage, 20 + slot)
                    send_part(array, 4 * right + quarter + 1, partner, stage, 22 + slot)
                for slot, quarter in enumerate((0, 2)):
                    wait_part(array, 4 * left + quarter + 1)
                    send_part(array, 4 * left + quarter + 1, partner, stage, 24 + slot)
                    wait_part(array, 4 * right + quarter)
                    send_part(array, 4 * right + quarter, partner, stage, 26 + slot)
                for quarter in range(4):
                    wait_part(array, 4 * across + quarter)
                    send_part(array, 4 * across + quarter, partner, stage, 28 + quarter)

        @pl.when((row < last) & (row >= 1))
        def _():
            wait_sent(0, range(4))

        for stage in range(1, levels):
            @pl.when(row + 2**stage < rows_total)
            def _(stage=stage):
                wait_sent(stage, range(4, 32))
                if stage < levels - 1:
                    @pl.when(row >= 2**stage)
                    def _():
                        wait_sent(stage, range(4))

        copy(landed, landed, send_sem.at[0, 0], misc_sem.at[0], partner).wait_recv()
        o_ref[0] = landed[...]

    @pl.when(core == 1)
    def _():
        def pass_sum(stage):
            @pl.when(row >= 2**stage)
            def _():
                for quarter in range(4):
                    copy(
                        sums.at[stage, pl.ds(quarter * piece, piece)],
                        part(maps_end + stage + 1, 4 * ring + quarter),
                        send_sem.at[stage, 12 + quarter],
                        full_sem.at[maps_end + stage + 1, 4 * ring + quarter],
                        (row - 2**stage, col),
                    ).start()

        def term(array, place):
            rows = rows_of(place, block)
            high, low = split(full[array, rows])
            return product3(t_high[:, rows], t_low[:, rows], high, low)

        split_turned(0)
        sums[0] = product3(t_high[...], t_low[...], m_high[...], m_low[...])

        @pl.when(row < last)
        def _():
            pass_sum(0)

        rest_of_weight()
        for place in range(4):
            weight_rows(place)
        split_full(1)
        split_turned(1)

        @pl.when(row == last)
        def _():
            total = term(b_array, 0) + term(b_array, 1) + term(b_array, 2) + term(b_array, 3)
            sums[0] = sums[0] + times_full(total)
            pass_sum(0)

        for stage in range(1, levels + 1):
            step = 2 ** (stage - 1)
            array = maps_end + stage

            @pl.when(row + step < rows_total)
            def _(stage=stage, step=step, array=array):
                if stage > 1:
                    for number in range(16):
                        wait_part(stage, number)
                    split_full(stage)
                    split_turned(stage)
                for quarter in range(4):
                    wait_part(array, 4 * ring + quarter)
                    send_part(array, 4 * ring + quarter, to_right, stage, quarter)
                    send_part(array, 4 * ring + quarter, to_left, stage, 4 + quarter)
                total = term(array, ring)
                for slot, quarter in enumerate((0, 2)):
                    wait_part(array, 4 * left + quarter)
                    send_part(array, 4 * left + quarter, to_right, stage, 8 + slot)
                    wait_part(array, 4 * right + quarter)
                    wait_part(array, 4 * left + quarter + 1)
                    wait_part(array, 4 * right + quarter + 1)
                    send_part(array, 4 * right + quarter + 1, to_left, stage, 10 + slot)
                total = total + term(array, left) + term(array, right)
                for quarter in range(4):
                    wait_part(array, 4 * across + quarter)
                total = total + term(array, across)
                sums[stage] = sums[stage - 1] + times_full(total)

            @pl.when(row + step >= rows_total)
            def _(stage=stage):
                sums[stage] = sums[stage - 1]

            if stage < levels:
                pass_sum(stage)

        for half in range(2):
            copy(
                sums.at[levels, pl.ds(half * piece, piece)],
                landed.at[pl.ds(half * piece, piece)],
                send_sem.at[0, half], misc_sem.at[0], partner,
            ).start()
        o_ref[0] = sums[levels, pl.ds(chunk, chunk)]

        for stage in range(levels):
            @pl.when(row >= 2**stage)
            def _(stage=stage):
                wait_sent(stage, range(12, 16))

        for stage in range(1, levels + 1):
            @pl.when(row + 2 ** (stage - 1) < rows_total)
            def _(stage=stage):
                wait_sent(stage, range(12))

        wait_sent(0, range(2))

    wait_sent(at_d, range(14))
    wait_sent(at_s, range(14))

    @pl.when(row == last)
    def _():
        wait_sent(at_b, range(14))


def on_device(rows_total, diag_tiles, sub_tiles, boundary):
    size = diag_tiles.shape[-1]
    levels = rows_total.bit_length() - 1
    chunk = size // 8
    block = size // 4
    arrays = 2 * levels + 3
    return pl.pallas_call(
        functools.partial(kernel, rows_total, levels),
        out_shape=jax.ShapeDtypeStruct(diag_tiles.shape, F32),
        in_specs=[pl.BlockSpec(memory_space=pl.ANY)] * 3,
        out_specs=pl.BlockSpec(memory_space=pltpu.VMEM),
        scratch_shapes=[
            pltpu.VMEM((arrays, size, size), F32),
            pltpu.VMEM((levels + 1, block, size), F32),
            pltpu.VMEM((chunk, size), F32),
            pltpu.VMEM((size, size), BF16),
            pltpu.VMEM((size, size), BF16),
            pltpu.VMEM((block, size), BF16),
            pltpu.VMEM((block, size), BF16),
            pltpu.SemaphoreType.DMA((arrays, 16)),
            pltpu.SemaphoreType.DMA((4,)),
            pltpu.SemaphoreType.DMA((levels + 4, 32)),
        ],
        compiler_params=pltpu.CompilerParams(
            collective_id=0, has_side_effects=True, vmem_limit_bytes=60 * 1024 * 1024
        ),
    )(diag_tiles, sub_tiles, boundary)


def solution(mesh):
    spec = jax.sharding.PartitionSpec
    tiles = spec("row", "col", None)
    return jax.shard_map(
        functools.partial(on_device, mesh.shape["row"]),
        mesh=mesh,
        in_specs=(tiles, tiles, spec("col", None)),
        out_specs=tiles,
        check_vma=False,
    )
```

```python
import functools

import jax
import jax.numpy as jnp
from jax import lax
from jax.experimental import pallas as pl
from jax.experimental.pallas import tpu as pltpu

MESH = pl.DeviceIdType.MESH
BF16 = jnp.bfloat16
F32 = jnp.float32


def split(value):
    high = value.astype(BF16)
    low = (value - high.astype(F32)).astype(BF16)
    return high, low


def dot(left, right):
    return jnp.dot(left, right, preferred_element_type=F32)


def product3(left_high, left_low, right_high, right_low):
    rows = left_high.shape[0]
    both = dot(jnp.concatenate([left_high, left_low], axis=0), right_high)
    return both[:rows] + both[rows:] + dot(left_high, right_low)


def kernel(
    rows_total, levels, d_ref, s_ref, b_ref, o_ref,
    full, sums, m_high, m_low, t_high, t_low, a_high, a_low,
    input_sem, ring_sem, entry_sem, map_sem, misc_sem, send_sem,
):
    maps_end = levels
    s_array = 2 * levels + 1
    b_array = 2 * levels + 2
    size = d_ref.shape[-1]
    chunk = size // 8
    block = size // 4
    piece = size // 16
    row = lax.axis_index("row")
    col = lax.axis_index("col")
    ring = col // 2
    core = col % 2
    right = (ring + 1) % 4
    left = (ring + 3) % 4
    across = (ring + 2) % 4
    partner = (row, 2 * ring + (1 - core))
    to_right = (row, 2 * right + core)
    to_left = (row, 2 * left + core)
    last = rows_total - 1

    def rows_of(number, length):
        return pl.ds(pl.multiple_of(number * length, length), length)

    def copy(src, dst, send, recv, device):
        return pltpu.make_async_remote_copy(
            src_ref=src, dst_ref=dst, send_sem=send, recv_sem=recv,
            device_id=device, device_id_type=MESH,
        )

    def wait_for(ref, sem):
        copy(ref, ref, send_sem.at[0, 0], sem, partner).wait_recv()

    def wait_sent(sem, arrays, rows):
        some = full.at[pl.ds(0, arrays), pl.ds(0, rows)]
        copy(some, some, sem, misc_sem.at[0], partner).wait_send()

    mine = 2 * ring + core
    own_rows = rows_of(mine, chunk)
    inputs = ((d_ref.at[0], 0), (s_ref.at[0], s_array), (b_ref, b_array))
    fetches = [
        pltpu.make_async_copy(ref, full.at[array, own_rows], misc_sem.at[1 + k])
        for k, (ref, array) in enumerate(inputs)
    ]
    for fetch in fetches:
        fetch.start()

    barrier = pltpu.get_barrier_semaphore()
    greeted = [partner, to_right, to_left]
    for level in range(levels):
        step = 2**level
        greeted.append(((row + step) % rows_total, col))
        greeted.append(((row + rows_total - step) % rows_total, col))
    for device in greeted:
        pl.semaphore_signal(barrier, inc=1, device_id=device, device_id_type=MESH)
    for fetch in fetches:
        fetch.wait()
    pl.semaphore_wait(barrier, len(greeted))

    def half_of(kind, place, half):
        return full.at[inputs[kind][1], rows_of(4 * place + 2 * core + half, piece)]

    def send_half(kind, place, half, device, slot):
        here = half_of(kind, place, half)
        copy(here, here, send_sem.at[levels + 1 + kind, 0], input_sem.at[kind, slot], device).start()

    def wait_half(kind, place, half, slot):
        wait_for(half_of(kind, place, half), input_sem.at[kind, slot])

    def gather_own(kind):
        for half in range(2):
            send_half(kind, ring, half, to_right, half)
            send_half(kind, ring, 1 - half, to_left, 2 + 1 - half)
        here = full.at[inputs[kind][1], own_rows]
        copy(here, here, send_sem.at[levels + 1 + kind, 0], input_sem.at[kind, 6], partner).start()

    def gather_near(kind):
        wait_half(kind, left, 0, 0)
        send_half(kind, left, 0, to_right, 4)
        wait_half(kind, right, 1, 3)
        send_half(kind, right, 1, to_left, 5)
        send_half(kind, left, 0, partner, 7)
        send_half(kind, right, 1, partner, 7)
        wait_half(kind, left, 1, 1)
        send_half(kind, left, 1, partner, 7)
        wait_half(kind, right, 0, 2)
        send_half(kind, right, 0, partner, 7)

    def gather_far(kind):
        for half in range(2):
            wait_half(kind, across, half, 4 + half)
            send_half(kind, across, half, partner, 7)

    def gather_beside(kind):
        wait_for(full.at[0, pl.ds(0, chunk)], input_sem.at[kind, 6])

    def gather_others(kind):
        wait_for(full.at[0, pl.ds(0, 3 * chunk)], input_sem.at[kind, 7])

    gather_own(0)
    gather_near(0)
    gather_own(1)
    gather_far(0)
    gather_near(1)

    @pl.when(row == last)
    def _():
        gather_own(2)

    gather_beside(0)
    gather_others(0)

    def split_full(array):
        for place in range(4):
            rows = pl.ds(place * block, block)
            m_high[rows], m_low[rows] = split(full[array, rows])

    def split_turned(array):
        t_high[...], t_low[...] = split(full[array, :, rows_of(ring, block)].T)

    def times_full(value):
        high, low = split(value)
        return product3(high, low, m_high[...], m_low[...])

    def weight_rows(place):
        rows = rows_of(place, block)
        full[1, rows] = times_full(full[s_array, rows])

    split_full(0)

    @pl.when(core == 0)
    def _():
        def quarter_of(array, place, quarter):
            return full.at[array, rows_of(4 * place + quarter, piece)]

        def pass_map(stage):
            @pl.when(row >= 2**stage)
            def _():
                for quarter in range(4):
                    copy(
                        quarter_of(stage + 1, ring, quarter),
                        quarter_of(maps_end + stage + 1, ring, quarter),
                        send_sem.at[stage, 1], entry_sem.at[stage + 1, quarter],
                        (row - 2**stage, col),
                    ).start()

        gather_beside(1)

        @pl.when(row < last)
        def _():
            weight_rows(ring)
            pass_map(0)

        gather_far(1)

        @pl.when(row == last)
        def _():
            gather_near(2)
            gather_far(2)
            gather_beside(2)
            gather_others(2)

        gather_others(1)

        @pl.when(row < last)
        def _():
            for place in (left, right, across):
                weight_rows(place)

        for stage in range(1, levels):
            @pl.when(row + 2**stage < rows_total)
            def _(stage=stage):
                array = stage + 1

                def send(place, quarter, device, slot):
                    here = quarter_of(array, place, quarter)
                    copy(
                        here, here, send_sem.at[stage, 0], ring_sem.at[stage % 2, slot], device
                    ).start()

                def hand_over(place, quarter):
                    here = quarter_of(array, place, quarter)
                    copy(here, here, send_sem.at[stage, 2], map_sem.at[stage], partner).start()

                def wait(place, quarter, slot):
                    wait_for(quarter_of(array, place, quarter), ring_sem.at[stage % 2, slot])

                split_full(stage)
                for quarter in range(4):
                    wait_for(
                        quarter_of(maps_end + stage, ring, quarter), entry_sem.at[stage, quarter]
                    )
                rows = rows_of(ring, block)
                full[array, rows] = times_full(full[maps_end + stage, rows])
                for one, other in ((0, 1), (2, 3), (1, 0), (3, 2)):
                    send(ring, one, to_right, one)
                    send(ring, other, to_left, 4 + other)
                if stage < levels - 1:
                    pass_map(stage)
                for quarter in range(4):
                    hand_over(ring, quarter)
                for quarter in (0, 2):
                    wait(left, quarter, quarter)
                    send(left, quarter, to_right, 8 + quarter)
                    wait(right, quarter + 1, 5 + quarter)
                    send(right, quarter + 1, to_left, 9 + quarter)
                    hand_over(left, quarter)
                    hand_over(right, quarter + 1)
                for quarter in (0, 2):
                    wait(left, quarter + 1, quarter + 1)
                    hand_over(left, quarter + 1)
                    wait(right, quarter, 4 + quarter)
                    hand_over(right, quarter)
                for quarter in range(4):
                    wait(across, quarter, 8 + quarter)
                    hand_over(across, quarter)

        @pl.when((row < last) & (row >= 1))
        def _():
            wait_sent(send_sem.at[0, 1], 1, block)

        for stage in range(1, levels):
            @pl.when(row + 2**stage < rows_total)
            def _(stage=stage):
                wait_sent(send_sem.at[stage, 0], 3, block)
                wait_sent(send_sem.at[stage, 2], 1, size)
                if stage < levels - 1:
                    @pl.when(row >= 2**stage)
                    def _():
                        wait_sent(send_sem.at[stage, 1], 1, block)

        wait_for(o_ref.at[0], misc_sem.at[0])

    @pl.when(core == 1)
    def _():
        def block_of(array, place, number, half=None):
            rows = rows_of(place, block) if half is None else rows_of(2 * place + half, chunk)
            return array, rows, rows_of((place + number) % 4, block)

        def if_sent(place, number, act):
            if number < 2:
                act()
            else:
                pl.when(place < 2)(act)

        def pass_sum(stage):
            target = maps_end + stage + 1

            @pl.when(row >= 2**stage)
            def _():
                for number in range(3):
                    @functools.partial(if_sent, ring, number)
                    def _(number=number):
                        for half in range(2):
                            there = block_of(target, ring, number, half)
                            copy(
                                sums.at[stage, pl.ds(half * chunk, chunk), there[2]],
                                full.at[there],
                                send_sem.at[stage, 1], entry_sem.at[stage + 1, 2 * number + half],
                                (row - 2**stage, col),
                            ).start()

        def put(array, place, number):
            there = block_of(array, place, number)
            value = full[there]
            a_high[there[1:]], a_low[there[1:]] = split(value)
            if number:
                turned = (there[2], there[1])
                a_high[turned], a_low[turned] = split(value.T)

        def compose(before):
            inner = product3(t_high[...], t_low[...], a_high[...], a_low[...])
            return before + times_full(inner)

        split_turned(0)
        sums[0] = product3(t_high[...], t_low[...], m_high[...], m_low[...])

        @pl.when(row < last)
        def _():
            pass_sum(0)

        gather_far(1)
        gather_beside(1)
        gather_others(1)

        @pl.when(row == last)
        def _():
            gather_near(2)

        for place in range(4):
            weight_rows(place)
        split_full(1)
        split_turned(1)

        @pl.when(row == last)
        def _():
            gather_far(2)
            gather_beside(2)
            gather_others(2)
            for place in range(4):
                rows = pl.ds(place * block, block)
                a_high[rows], a_low[rows] = split(full[b_array, rows])
            sums[0] = compose(sums[0])
            pass_sum(0)

        for stage in range(1, levels + 1):
            step = 2 ** (stage - 1)
            array = maps_end + stage

            @pl.when(row + step < rows_total)
            def _(stage=stage, step=step, array=array):
                def send(place, number, half, device, slot):
                    here = full.at[block_of(array, place, number, half)]
                    copy(
                        here, here, send_sem.at[stage, 0],
                        ring_sem.at[stage % 2, slot + 2 * number + half], device,
                    ).start()

                def wait(place, number, half, slot):
                    here = full.at[block_of(array, place, number, half)]
                    wait_for(here, ring_sem.at[stage % 2, slot + 2 * number + half])

                if stage > 1:
                    wait_for(full.at[stage], map_sem.at[stage - 1])
                    split_full(stage)
                    split_turned(stage)
                for number in range(3):
                    @functools.partial(if_sent, ring, number)
                    def _(number=number):
                        for half in range(2):
                            here = full.at[block_of(array, ring, number, half)]
                            wait_for(here, entry_sem.at[stage, 2 * number + half])
                            send(ring, number, half, to_right, 0)
                            send(ring, number, half, to_left, 6)
                for number in range(3):
                    if_sent(ring, number, functools.partial(put, array, ring, number))
                for number in range(3):
                    @functools.partial(if_sent, left, number)
                    def _(number=number):
                        wait(left, number, 0, 0)
                        send(left, number, 0, to_right, 12)

                    @functools.partial(if_sent, right, number)
                    def _(number=number):
                        wait(right, number, 1, 6)
                        send(right, number, 1, to_left, 12)
                for number in range(3):
                    @functools.partial(if_sent, left, number)
                    def _(number=number):
                        wait(left, number, 1, 0)
                        put(array, left, number)

                    @functools.partial(if_sent, right, number)
                    def _(number=number):
                        wait(right, number, 0, 6)
                        put(array, right, number)
                for number in range(3):
                    @functools.partial(if_sent, across, number)
                    def _(number=number):
                        wait(across, number, 0, 12)
                        wait(across, number, 1, 12)
                        put(array, across, number)
                sums[stage] = compose(sums[stage - 1])

            @pl.when(row + step >= rows_total)
            def _(stage=stage):
                sums[stage] = sums[stage - 1]

            if stage < levels:
                pass_sum(stage)

        upper = copy(
            sums.at[levels, pl.ds(0, chunk)], o_ref.at[0],
            send_sem.at[0, 0], misc_sem.at[0], partner,
        )
        lower = pltpu.make_async_copy(
            sums.at[levels, pl.ds(chunk, chunk)], o_ref.at[0], misc_sem.at[1]
        )
        upper.start()
        lower.start()

        def wait_blocks(sem, first, others):
            @pl.when(ring < 2)
            def _():
                wait_sent(sem, 1, first * piece // 2)

            @pl.when(ring >= 2)
            def _():
                wait_sent(sem, 1, others * piece // 2)

        for stage in range(levels):
            @pl.when(row >= 2**stage)
            def _(stage=stage):
                wait_blocks(send_sem.at[stage, 1], 6, 4)

        for stage in range(1, levels + 1):
            @pl.when(row + 2 ** (stage - 1) < rows_total)
            def _(stage=stage):
                wait_blocks(send_sem.at[stage, 0], 17, 13)

        lower.wait()
        upper.wait_send()

    for kind in range(2):
        wait_sent(send_sem.at[levels + 1 + kind, 0], 1, 7 * chunk)

    @pl.when(row == last)
    def _():
        wait_sent(send_sem.at[levels + 3, 0], 1, 7 * chunk)


def on_device(rows_total, diag_tiles, sub_tiles, boundary):
    size = diag_tiles.shape[-1]
    levels = rows_total.bit_length() - 1
    block = size // 4
    arrays = 2 * levels + 3
    return pl.pallas_call(
        functools.partial(kernel, rows_total, levels),
        out_shape=jax.ShapeDtypeStruct(diag_tiles.shape, F32),
        in_specs=[pl.BlockSpec(memory_space=pl.ANY)] * 3,
        out_specs=pl.BlockSpec(memory_space=pl.ANY),
        scratch_shapes=[
            pltpu.VMEM((arrays, size, size), F32),
            pltpu.VMEM((levels + 1, block, size), F32),
            pltpu.VMEM((size, size), BF16),
            pltpu.VMEM((size, size), BF16),
            pltpu.VMEM((block, size), BF16),
            pltpu.VMEM((block, size), BF16),
            pltpu.VMEM((size, size), BF16),
            pltpu.VMEM((size, size), BF16),
            pltpu.SemaphoreType.DMA((3, 8)),
            pltpu.SemaphoreType.DMA((2, 18)),
            pltpu.SemaphoreType.DMA((levels + 1, 6)),
            pltpu.SemaphoreType.DMA((levels,)),
            pltpu.SemaphoreType.DMA((4,)),
            pltpu.SemaphoreType.DMA((levels + 4, 3)),
        ],
        compiler_params=pltpu.CompilerParams(
            collective_id=0, has_side_effects=True, vmem_limit_bytes=60 * 1024 * 1024
        ),
    )(diag_tiles, sub_tiles, boundary)


def solution(mesh):
    spec = jax.sharding.PartitionSpec
    tiles = spec("row", "col", None)
    return jax.shard_map(
        functools.partial(on_device, mesh.shape["row"]),
        mesh=mesh,
        in_specs=(tiles, tiles, spec("col", None)),
        out_specs=tiles,
        check_vma=False,
    )
```

```python
import functools

import jax
import jax.numpy as jnp
from jax import lax
from jax.experimental import pallas as pl
from jax.experimental.pallas import tpu as pltpu

MESH = pl.DeviceIdType.MESH
BF16 = jnp.bfloat16
F32 = jnp.float32


def split(value):
    high = value.astype(BF16)
    low = (value - high.astype(F32)).astype(BF16)
    return high, low


def dot(left, right):
    return jnp.dot(left, right, preferred_element_type=F32)


def product3(left_high, left_low, right_high, right_low):
    rows = left_high.shape[0]
    both = dot(jnp.concatenate([left_high, left_low], axis=0), right_high)
    return both[:rows] + both[rows:] + dot(left_high, right_low)


def kernel(
    rows_total, levels, d_ref, s_ref, b_ref, o_ref,
    full, sums, halves, m_high, m_low, t_high, t_low, a_high, a_low,
    input_sem, ring_sem, entry_sem, map_sem, misc_sem, send_sem,
):
    maps_end = levels
    s_array = 2 * levels + 1
    b_array = 2 * levels + 2
    size = d_ref.shape[-1]
    chunk = size // 8
    block = size // 4
    piece = size // 16
    row = lax.axis_index("row")
    col = lax.axis_index("col")
    ring = col // 2
    core = col % 2
    right = (ring + 1) % 4
    left = (ring + 3) % 4
    across = (ring + 2) % 4
    partner = (row, 2 * ring + (1 - core))
    to_right = (row, 2 * right + core)
    to_left = (row, 2 * left + core)
    last = rows_total - 1

    def rows_of(number, length):
        return pl.ds(pl.multiple_of(number * length, length), length)

    def copy(src, dst, send, recv, device):
        return pltpu.make_async_remote_copy(
            src_ref=src, dst_ref=dst, send_sem=send, recv_sem=recv,
            device_id=device, device_id_type=MESH,
        )

    def wait_for(ref, sem):
        copy(ref, ref, send_sem.at[0, 0], sem, partner).wait_recv()

    def wait_sent(sem, arrays, rows):
        some = full.at[pl.ds(0, arrays), pl.ds(0, rows)]
        copy(some, some, sem, misc_sem.at[0], partner).wait_send()

    mine = 2 * ring + core
    own_rows = rows_of(mine, chunk)
    inputs = ((d_ref.at[0], 0), (s_ref.at[0], s_array), (b_ref, b_array))
    fetches = [
        pltpu.make_async_copy(ref, full.at[array, own_rows], misc_sem.at[1 + k])
        for k, (ref, array) in enumerate(inputs)
    ]
    for fetch in fetches:
        fetch.start()

    barrier = pltpu.get_barrier_semaphore()
    greeted = [partner, to_right, to_left]
    for level in range(levels):
        step = 2**level
        greeted.append(((row + step) % rows_total, col))
        greeted.append(((row + rows_total - step) % rows_total, col))
    for device in greeted:
        pl.semaphore_signal(barrier, inc=1, device_id=device, device_id_type=MESH)
    for fetch in fetches:
        fetch.wait()
    pl.semaphore_wait(barrier, len(greeted))

    def input_piece(kind, place, number):
        return full.at[inputs[kind][1], rows_of(4 * place + number, piece)]

    def send_input(kind, place, number, device, slot):
        here = input_piece(kind, place, number)
        copy(here, here, send_sem.at[levels + 1 + kind, 0], input_sem.at[kind, slot], device).start()

    def wait_input(kind, place, number, slot):
        wait_for(input_piece(kind, place, number), input_sem.at[kind, slot])

    def hand_own(kind):
        here = full.at[inputs[kind][1], own_rows]
        copy(here, here, send_sem.at[levels + 1 + kind, 1], input_sem.at[kind, 12], partner).start()

    def gather_own(kind, numbers):
        for number in numbers:
            send_input(kind, ring, number, to_right, number)
        for number in reversed(numbers):
            send_input(kind, ring, number, to_left, 4 + number)

    def gather_near(kind):
        for number in (2, 0):
            wait_input(kind, left, number, number)
            send_input(kind, left, number, to_right, 8 + number)
            wait_input(kind, right, number + 1, 5 + number)
            send_input(kind, right, number + 1, to_left, 9 + number)
            send_input(kind, left, number, partner, 13)
            send_input(kind, right, number + 1, partner, 13)
        for number in (2, 0):
            wait_input(kind, left, number + 1, number + 1)
            send_input(kind, left, number + 1, partner, 13)
            wait_input(kind, right, number, 4 + number)
            send_input(kind, right, number, partner, 13)

    def gather_far(kind):
        for number in (2, 3, 0, 1):
            wait_input(kind, across, number, 8 + number)
            send_input(kind, across, number, partner, 13)

    def wait_beside(kind):
        wait_for(full.at[0, pl.ds(0, chunk)], input_sem.at[kind, 12])

    def wait_others(kind):
        wait_for(full.at[0, pl.ds(0, 3 * block)], input_sem.at[kind, 13])

    def split_full(array):
        for place in range(4):
            rows = pl.ds(place * block, block)
            m_high[rows], m_low[rows] = split(full[array, rows])

    def split_turned(array):
        t_high[...], t_low[...] = split(full[array, :, rows_of(ring, block)].T)

    def times_full(value):
        high, low = split(value)
        return product3(high, low, m_high[...], m_low[...])

    def weight_rows(place):
        rows = rows_of(place, block)
        full[1, rows] = times_full(full[s_array, rows])

    @pl.when(core == 0)
    def _():
        hand_own(0)
        hand_own(1)

        @pl.when(row == last)
        def _():
            hand_own(2)

        def quarter_of(array, place, quarter):
            return full.at[array, rows_of(4 * place + quarter, piece)]

        def pass_map(stage):
            @pl.when(row >= 2**stage)
            def _():
                for quarter in range(4):
                    copy(
                        quarter_of(stage + 1, ring, quarter),
                        quarter_of(maps_end + stage + 1, ring, quarter),
                        send_sem.at[stage, 1], entry_sem.at[stage + 1, quarter],
                        (row - 2**stage, col),
                    ).start()

        wait_beside(0)
        wait_beside(1)
        wait_others(0)

        @pl.when(row < last)
        def _():
            split_full(0)
            weight_rows(ring)
            pass_map(0)

        wait_others(1)

        @pl.when(row < last)
        def _():
            for place in (left, right, across):
                weight_rows(place)

        for stage in range(1, levels):
            @pl.when(row + 2**stage < rows_total)
            def _(stage=stage):
                array = stage + 1

                def eighth_of(place, eighth):
                    return full.at[array, rows_of(8 * place + eighth, piece // 2)]

                def send(place, eighth, device, slot):
                    here = eighth_of(place, eighth)
                    copy(
                        here, here, send_sem.at[stage, 0], ring_sem.at[stage % 2, slot], device
                    ).start()

                def hand_over(place, eighth):
                    here = eighth_of(place, eighth)
                    copy(here, here, send_sem.at[stage, 2], map_sem.at[stage], partner).start()

                def wait(place, eighth, slot):
                    wait_for(eighth_of(place, eighth), ring_sem.at[stage % 2, slot])

                split_full(stage)
                for quarter in range(4):
                    wait_for(
                        quarter_of(maps_end + stage, ring, quarter), entry_sem.at[stage, quarter]
                    )
                rows = rows_of(ring, block)
                full[array, rows] = times_full(full[maps_end + stage, rows])
                for eighth in (0, 2, 4, 6, 1, 3, 5, 7):
                    other = eighth + 1 - 2 * (eighth % 2)
                    send(ring, eighth, to_right, eighth)
                    send(ring, other, to_left, 8 + other)
                if stage < levels - 1:
                    pass_map(stage)
                for eighth in range(8):
                    hand_over(ring, eighth)
                for eighth in (0, 2, 4, 6):
                    wait(left, eighth, eighth)
                    send(left, eighth, to_right, 16 + eighth)
                    wait(right, eighth + 1, 9 + eighth)
                    send(right, eighth + 1, to_left, 17 + eighth)
                    hand_over(left, eighth)
                    hand_over(right, eighth + 1)
                for eighth in (0, 2, 4, 6):
                    wait(left, eighth + 1, eighth + 1)
                    hand_over(left, eighth + 1)
                    wait(right, eighth, 8 + eighth)
                    hand_over(right, eighth)
                for eighth in range(8):
                    wait(across, eighth, 16 + eighth)
                    hand_over(across, eighth)

        @pl.when((row < last) & (row >= 1))
        def _():
            wait_sent(send_sem.at[0, 1], 1, block)

        for stage in range(1, levels):
            @pl.when(row + 2**stage < rows_total)
            def _(stage=stage):
                wait_sent(send_sem.at[stage, 0], 3, block)
                wait_sent(send_sem.at[stage, 2], 1, size)
                if stage < levels - 1:
                    @pl.when(row >= 2**stage)
                    def _():
                        wait_sent(send_sem.at[stage, 1], 1, block)

        wait_for(o_ref.at[0], misc_sem.at[0])

    @pl.when(core == 1)
    def _():
        def piece_of(array, place, number):
            if number < 4:
                first, second = 2 * place + number % 2, (place + number // 2) % 4
            else:
                first, second = 2 * (place % 2) + place // 2, place % 2 + 2
            return full.at[array, rows_of(first, chunk), rows_of(second, block)]

        def pass_sum(stage):
            target = maps_end + stage + 1

            @pl.when(row >= 2**stage)
            def _():
                def start(source, number):
                    copy(
                        source, piece_of(target, ring, number),
                        send_sem.at[stage, 1], entry_sem.at[stage + 1, number],
                        (row - 2**stage, col),
                    ).start()

                for number in range(4):
                    start(
                        sums.at[
                            stage, pl.ds(number % 2 * chunk, chunk),
                            rows_of((ring + number // 2) % 4, block),
                        ],
                        number,
                    )
                shared = sums[stage, :, rows_of(across, block)]

                @pl.when(ring < 2)
                def _():
                    halves[stage] = shared[:chunk]

                @pl.when(ring >= 2)
                def _():
                    halves[stage] = shared.T[chunk:]

                start(halves.at[stage], 4)

        def wait_passed(stage):
            @pl.when(row >= 2**stage)
            def _():
                wait_sent(send_sem.at[stage, 1], 1, 5 * piece // 2)

        def put(array, place, second, turn):
            rows, columns = rows_of(place, block), rows_of(second, block)
            value = full[array, rows, columns]
            a_high[rows, columns], a_low[rows, columns] = split(value)
            if turn:
                a_high[columns, rows], a_low[columns, rows] = split(value.T)

        def send_sum(stage, array, place, number, device, slot):
            here = piece_of(array, place, number)
            sent = send_sem.at[stage, 0] if stage <= levels else send_sem.at[levels + 1, 2]
            copy(here, here, sent, ring_sem.at[stage % 2, slot + number], device).start()

        def wait_sum(stage, array, place, number, slot):
            wait_for(piece_of(array, place, number), ring_sem.at[stage % 2, slot + number])

        def sum_own(stage, array, arrival):
            for number in range(5):
                arrival(number)
                send_sum(stage, array, ring, number, to_right, 0)
                send_sum(stage, array, ring, number, to_left, 5)
            put(array, ring, ring, False)
            put(array, ring, right, True)

        def sum_near(stage, array):
            for number in (0, 2, 4):
                wait_sum(stage, array, left, number, 0)
                send_sum(stage, array, left, number, to_right, 10)
                if number < 4:
                    wait_sum(stage, array, right, number + 1, 5)
                    send_sum(stage, array, right, number + 1, to_left, 10)
            wait_sum(stage, array, left, 1, 0)
            put(array, left, left, False)
            wait_sum(stage, array, right, 0, 5)
            put(array, right, right, False)
            wait_sum(stage, array, left, 3, 0)
            put(array, left, ring, True)
            wait_sum(stage, array, right, 2, 5)
            put(array, right, across, True)
            wait_sum(stage, array, right, 4, 5)
            put(array, left % 2, left % 2 + 2, True)

        def sum_far(stage, array):
            for number in range(5):
                wait_sum(stage, array, across, number, 10)
                if number == 1:
                    put(array, across, across, False)
                if number == 3:
                    put(array, across, left, True)
            put(array, ring % 2, ring % 2 + 2, True)

        def compose(before):
            inner = product3(t_high[...], t_low[...], a_high[...], a_low[...])
            return before + times_full(inner)

        gather_own(0, (2, 3))
        hand_own(0)
        wait_beside(0)
        gather_own(0, (0, 1))
        gather_near(0)
        hand_own(1)
        wait_beside(1)
        gather_own(1, (2, 3, 0, 1))

        @pl.when(row == last)
        def _():
            wait_beside(2)

            @pl.when(ring >= 2)
            def _():
                shared = full[b_array, rows_of(ring, block), rows_of(ring - 2, block)]
                full[b_array, rows_of(2 * (ring - 2) + 1, chunk), rows_of(ring, block)] = (
                    shared.T[chunk:]
                )

            sum_own(levels + 1, b_array, lambda number: None)

        gather_far(0)
        split_full(0)
        split_turned(0)
        sums[0] = product3(t_high[...], t_low[...], m_high[...], m_low[...])

        @pl.when(row < last)
        def _():
            pass_sum(0)

        gather_near(1)

        @pl.when(row == last)
        def _():
            sum_near(levels + 1, b_array)

        gather_far(1)
        for place in range(4):
            weight_rows(place)
        split_full(1)
        split_turned(1)

        @pl.when(row == last)
        def _():
            sum_far(levels + 1, b_array)
            sums[0] = compose(sums[0])
            pass_sum(0)

        for stage in range(1, levels + 1):
            step = 2 ** (stage - 1)
            array = maps_end + stage

            @pl.when(row + step < rows_total)
            def _(stage=stage, step=step, array=array):
                if stage > 1:
                    wait_for(full.at[stage], map_sem.at[stage - 1])
                    split_full(stage)
                    split_turned(stage)

                def arrival(number):
                    wait_for(piece_of(array, ring, number), entry_sem.at[stage, number])

                sum_own(stage, array, arrival)
                sum_near(stage, array)
                sum_far(stage, array)
                sums[stage] = compose(sums[stage - 1])

            @pl.when(row + step >= rows_total)
            def _(stage=stage):
                sums[stage] = sums[stage - 1]
                wait_passed(stage - 1)

            if stage < levels:
                pass_sum(stage)

        upper = copy(
            sums.at[levels, pl.ds(0, chunk)], o_ref.at[0],
            send_sem.at[0, 0], misc_sem.at[0], partner,
        )
        lower = pltpu.make_async_copy(
            sums.at[levels, pl.ds(chunk, chunk)], o_ref.at[0], misc_sem.at[1]
        )
        upper.start()
        lower.start()

        for stage in range(levels):
            @pl.when(row + 2**stage < rows_total)
            def _(stage=stage):
                wait_passed(stage)

        for stage in range(1, levels + 1):
            @pl.when(row + 2 ** (stage - 1) < rows_total)
            def _(stage=stage):
                wait_sent(send_sem.at[stage, 0], 1, 15 * piece // 2)

        @pl.when(row == last)
        def _():
            wait_sent(send_sem.at[levels + 1, 2], 1, 15 * piece // 2)

        for kind in range(2):
            wait_sent(send_sem.at[levels + 1 + kind, 0], 2, 12 * piece)
        lower.wait()
        upper.wait_send()

    for kind in range(2):
        wait_sent(send_sem.at[levels + 1 + kind, 1], 1, chunk)

    @pl.when((row == last) & (core == 0))
    def _():
        wait_sent(send_sem.at[levels + 3, 1], 1, chunk)


def on_device(rows_total, diag_tiles, sub_tiles, boundary):
    size = diag_tiles.shape[-1]
    levels = rows_total.bit_length() - 1
    block = size // 4
    arrays = 2 * levels + 3
    return pl.pallas_call(
        functools.partial(kernel, rows_total, levels),
        out_shape=jax.ShapeDtypeStruct(diag_tiles.shape, F32),
        in_specs=[pl.BlockSpec(memory_space=pl.ANY)] * 3,
        out_specs=pl.BlockSpec(memory_space=pl.ANY),
        scratch_shapes=[
            pltpu.VMEM((arrays, size, size), F32),
            pltpu.VMEM((levels + 1, block, size), F32),
            pltpu.VMEM((levels, size // 8, block), F32),
            pltpu.VMEM((size, size), BF16),
            pltpu.VMEM((size, size), BF16),
            pltpu.VMEM((block, size), BF16),
            pltpu.VMEM((block, size), BF16),
            pltpu.VMEM((size, size), BF16),
            pltpu.VMEM((size, size), BF16),
            pltpu.SemaphoreType.DMA((3, 14)),
            pltpu.SemaphoreType.DMA((2, 24)),
            pltpu.SemaphoreType.DMA((levels + 1, 5)),
            pltpu.SemaphoreType.DMA((levels,)),
            pltpu.SemaphoreType.DMA((4,)),
            pltpu.SemaphoreType.DMA((levels + 4, 3)),
        ],
        compiler_params=pltpu.CompilerParams(
            collective_id=0, has_side_effects=True, vmem_limit_bytes=60 * 1024 * 1024
        ),
    )(diag_tiles, sub_tiles, boundary)


def solution(mesh):
    spec = jax.sharding.PartitionSpec
    tiles = spec("row", "col", None)
    return jax.shard_map(
        functools.partial(on_device, mesh.shape["row"]),
        mesh=mesh,
        in_specs=(tiles, tiles, spec("col", None)),
        out_specs=tiles,
        check_vma=False,
    )
```

```python
import functools

import jax
import jax.numpy as jnp
from jax import lax
from jax.experimental import pallas as pl
from jax.experimental.pallas import tpu as pltpu

MESH = pl.DeviceIdType.MESH
BF16 = jnp.bfloat16
F32 = jnp.float32


def split(value):
    high = value.astype(BF16)
    low = (value - high.astype(F32)).astype(BF16)
    return high, low


def dot(left, right):
    return jnp.dot(left, right, preferred_element_type=F32)


def product3(left_high, left_low, right_high, right_low):
    rows = left_high.shape[0]
    both = dot(jnp.concatenate([left_high, left_low], axis=0), right_high)
    return both[:rows] + both[rows:] + dot(left_high, right_low)


def kernel(
    rows_total, levels, d_ref, s_ref, b_ref, o_ref,
    full, sums, halves, m_high, m_low, t_high, t_low, a_high, a_low,
    input_sem, ring_sem, entry_sem, map_sem, misc_sem, send_sem, known_sem,
):
    maps_end = levels
    s_array = 2 * levels + 1
    b_array = 2 * levels + 2
    size = d_ref.shape[-1]
    chunk = size // 8
    block = size // 4
    piece = size // 16
    row = lax.axis_index("row")
    col = lax.axis_index("col")
    ring = col // 2
    core = col % 2
    right = (ring + 1) % 4
    left = (ring + 3) % 4
    across = (ring + 2) % 4
    partner = (row, 2 * ring + (1 - core))
    to_right = (row, 2 * right + core)
    to_left = (row, 2 * left + core)
    last = rows_total - 1

    def rows_of(number, length):
        return pl.ds(pl.multiple_of(number * length, length), length)

    def copy(src, dst, send, recv, device):
        return pltpu.make_async_remote_copy(
            src_ref=src, dst_ref=dst, send_sem=send, recv_sem=recv,
            device_id=device, device_id_type=MESH,
        )

    def wait_for(ref, sem):
        copy(ref, ref, send_sem.at[0, 0], sem, partner).wait_recv()

    def wait_sent(sem, arrays, rows):
        some = full.at[pl.ds(0, arrays), pl.ds(0, rows)]
        copy(some, some, sem, misc_sem.at[0], partner).wait_send()

    mine = 2 * ring + core
    own_rows = rows_of(mine, chunk)
    inputs = ((d_ref.at[0], 0), (s_ref.at[0], s_array), (b_ref, b_array))
    fetches = [
        pltpu.make_async_copy(ref, full.at[array, own_rows], misc_sem.at[1 + k])
        for k, (ref, array) in enumerate(inputs)
    ]
    for fetch in fetches:
        fetch.start()

    def rows_away(step):
        return ((row + step) % rows_total, col), ((row + rows_total - step) % rows_total, col)

    def tell(round):
        for device in rows_away(2**round):
            pl.semaphore_signal(
                known_sem.at[round], inc=1, device_id=device, device_id_type=MESH
            )

    def know(round):
        pl.semaphore_wait(known_sem.at[round], 2)
        if round < levels - 2:
            tell(round + 1)

    barrier = pltpu.get_barrier_semaphore()
    greeted = (partner, to_right, to_left, *rows_away(1))
    for device in greeted:
        pl.semaphore_signal(barrier, inc=1, device_id=device, device_id_type=MESH)
    for fetch in fetches:
        fetch.wait()
    pl.semaphore_wait(barrier, len(greeted))
    tell(0)

    def near_link_last(from_left, from_right):
        @pl.when(ring < 2)
        def _():
            from_right()
            from_left()

        @pl.when(ring >= 2)
        def _():
            from_left()
            from_right()

    def input_piece(kind, place, number):
        return full.at[inputs[kind][1], rows_of(4 * place + number, piece)]

    def send_input(kind, place, number, device, slot):
        here = input_piece(kind, place, number)
        copy(here, here, send_sem.at[levels + 1 + kind, 0], input_sem.at[kind, slot], device).start()

    def wait_input(kind, place, number, slot):
        wait_for(input_piece(kind, place, number), input_sem.at[kind, slot])

    def hand_own(kind):
        here = full.at[inputs[kind][1], own_rows]
        copy(here, here, send_sem.at[levels + 1 + kind, 1], input_sem.at[kind, 12], partner).start()

    def gather_own(kind, numbers):
        for number in numbers:
            send_input(kind, ring, number, to_right, number)
        for number in reversed(numbers):
            send_input(kind, ring, number, to_left, 4 + number)

    def gather_near(kind):
        def from_left():
            for number in (2, 0, 3, 1):
                wait_input(kind, left, number, number)
                if number % 2 == 0:
                    send_input(kind, left, number, to_right, 8 + number)
                send_input(kind, left, number, partner, 13)

        def from_right():
            for number in (3, 1, 2, 0):
                wait_input(kind, right, number, 4 + number)
                if number % 2 == 1:
                    send_input(kind, right, number, to_left, 8 + number)
                send_input(kind, right, number, partner, 13)

        near_link_last(from_left, from_right)

    def gather_far(kind):
        for number in (2, 3, 0, 1):
            wait_input(kind, across, number, 8 + number)
            send_input(kind, across, number, partner, 13)

    def wait_beside(kind):
        wait_for(full.at[0, pl.ds(0, chunk)], input_sem.at[kind, 12])

    def wait_others(kind):
        wait_for(full.at[0, pl.ds(0, 3 * block)], input_sem.at[kind, 13])

    def split_full(array):
        for place in range(4):
            rows = pl.ds(place * block, block)
            m_high[rows], m_low[rows] = split(full[array, rows])

    def split_turned(array):
        t_high[...], t_low[...] = split(full[array, :, rows_of(ring, block)].T)

    def times_full(value):
        high, low = split(value)
        return product3(high, low, m_high[...], m_low[...])

    def weight_rows(place):
        rows = rows_of(place, block)
        full[1, rows] = times_full(full[s_array, rows])

    @pl.when(core == 0)
    def _():
        hand_own(0)
        hand_own(1)

        @pl.when(row == last)
        def _():
            hand_own(2)

        def quarter_of(array, place, quarter):
            return full.at[array, rows_of(4 * place + quarter, piece)]

        def pass_map(stage):
            @pl.when(row >= 2**stage)
            def _():
                for quarter in range(4):
                    copy(
                        quarter_of(stage + 1, ring, quarter),
                        quarter_of(maps_end + stage + 1, ring, quarter),
                        send_sem.at[stage, 1], entry_sem.at[stage + 1, quarter],
                        (row - 2**stage, col),
                    ).start()

        wait_beside(0)
        know(0)
        wait_beside(1)
        know(1)
        wait_others(0)

        @pl.when(row < last)
        def _():
            split_full(0)
            weight_rows(ring)
            pass_map(0)

        for round in range(2, levels - 1):
            know(round)
        wait_others(1)

        @pl.when(row < last)
        def _():
            for place in (left, right, across):
                weight_rows(place)

        for stage in range(1, levels):
            @pl.when(row + 2**stage < rows_total)
            def _(stage=stage):
                array = stage + 1

                def eighth_of(place, eighth):
                    return full.at[array, rows_of(8 * place + eighth, piece // 2)]

                def send(place, eighth, device, slot):
                    here = eighth_of(place, eighth)
                    copy(
                        here, here, send_sem.at[stage, 0], ring_sem.at[stage % 2, slot], device
                    ).start()

                def hand_over(place, eighth):
                    here = eighth_of(place, eighth)
                    copy(here, here, send_sem.at[stage, 2], map_sem.at[stage], partner).start()

                def wait(place, eighth, slot):
                    wait_for(eighth_of(place, eighth), ring_sem.at[stage % 2, slot])

                split_full(stage)
                for quarter in range(4):
                    wait_for(
                        quarter_of(maps_end + stage, ring, quarter), entry_sem.at[stage, quarter]
                    )
                rows = rows_of(ring, block)
                full[array, rows] = times_full(full[maps_end + stage, rows])
                for eighth in (0, 2, 4, 6, 1, 3, 5, 7):
                    other = eighth + 1 - 2 * (eighth % 2)
                    send(ring, eighth, to_right, eighth)
                    send(ring, other, to_left, 8 + other)
                if stage < levels - 1:
                    pass_map(stage)
                for eighth in range(8):
                    hand_over(ring, eighth)

                def from_left():
                    for eighth in (0, 2, 4, 6):
                        wait(left, eighth, eighth)
                        send(left, eighth, to_right, 16 + eighth)
                        hand_over(left, eighth)

                def from_right():
                    for eighth in (1, 3, 5, 7):
                        wait(right, eighth, 8 + eighth)
                        send(right, eighth, to_left, 16 + eighth)
                        hand_over(right, eighth)

                near_link_last(from_left, from_right)
                for eighth in (0, 2, 4, 6):
                    wait(left, eighth + 1, eighth + 1)
                    hand_over(left, eighth + 1)
                    wait(right, eighth, 8 + eighth)
                    hand_over(right, eighth)
                for eighth in range(8):
                    wait(across, eighth, 16 + eighth)
                    hand_over(across, eighth)

        @pl.when((row < last) & (row >= 1))
        def _():
            wait_sent(send_sem.at[0, 1], 1, block)

        for stage in range(1, levels):
            @pl.when(row + 2**stage < rows_total)
            def _(stage=stage):
                wait_sent(send_sem.at[stage, 0], 3, block)
                wait_sent(send_sem.at[stage, 2], 1, size)
                if stage < levels - 1:
                    @pl.when(row >= 2**stage)
                    def _():
                        wait_sent(send_sem.at[stage, 1], 1, block)

        wait_for(o_ref.at[0], misc_sem.at[0])

    @pl.when(core == 1)
    def _():
        def piece_of(array, place, number):
            if number < 4:
                first, second = 2 * place + number % 2, (place + number // 2) % 4
            else:
                first, second = 2 * (place % 2) + place // 2, place % 2 + 2
            return full.at[array, rows_of(first, chunk), rows_of(second, block)]

        def pass_sum(stage):
            target = maps_end + stage + 1

            @pl.when(row >= 2**stage)
            def _():
                def start(source, number):
                    copy(
                        source, piece_of(target, ring, number),
                        send_sem.at[stage, 1], entry_sem.at[stage + 1, number],
                        (row - 2**stage, col),
                    ).start()

                for number in range(4):
                    start(
                        sums.at[
                            stage, pl.ds(number % 2 * chunk, chunk),
                            rows_of((ring + number // 2) % 4, block),
                        ],
                        number,
                    )
                shared = sums[stage, :, rows_of(across, block)]

                @pl.when(ring < 2)
                def _():
                    halves[stage] = shared[:chunk]

                @pl.when(ring >= 2)
                def _():
                    halves[stage] = shared.T[chunk:]

                start(halves.at[stage], 4)

        def wait_passed(stage):
            @pl.when(row >= 2**stage)
            def _():
                wait_sent(send_sem.at[stage, 1], 1, 5 * piece // 2)

        def put(array, place, second, turn):
            rows, columns = rows_of(place, block), rows_of(second, block)
            value = full[array, rows, columns]
            a_high[rows, columns], a_low[rows, columns] = split(value)
            if turn:
                a_high[columns, rows], a_low[columns, rows] = split(value.T)

        def send_sum(stage, array, place, number, device, slot):
            here = piece_of(array, place, number)
            sent = send_sem.at[stage, 0] if stage <= levels else send_sem.at[levels + 1, 2]
            copy(here, here, sent, ring_sem.at[stage % 2, slot + number], device).start()

        def wait_sum(stage, array, place, number, slot):
            wait_for(piece_of(array, place, number), ring_sem.at[stage % 2, slot + number])

        def sum_own(stage, array, arrival):
            for number in range(5):
                arrival(number)
                send_sum(stage, array, ring, number, to_right, 0)
                send_sum(stage, array, ring, number, to_left, 5)
            put(array, ring, ring, False)
            put(array, ring, right, True)

        def sum_near(stage, array):
            def from_left():
                for number in (0, 2, 4):
                    wait_sum(stage, array, left, number, 0)
                    send_sum(stage, array, left, number, to_right, 10)

            def from_right():
                for number in (1, 3):
                    wait_sum(stage, array, right, number, 5)
                    send_sum(stage, array, right, number, to_left, 10)

            near_link_last(from_left, from_right)
            wait_sum(stage, array, left, 1, 0)
            put(array, left, left, False)
            wait_sum(stage, array, right, 0, 5)
            put(array, right, right, False)
            wait_sum(stage, array, left, 3, 0)
            put(array, left, ring, True)
            wait_sum(stage, array, right, 2, 5)
            put(array, right, across, True)
            wait_sum(stage, array, right, 4, 5)
            put(array, left % 2, left % 2 + 2, True)

        def sum_far(stage, array):
            for number in range(5):
                wait_sum(stage, array, across, number, 10)
                if number == 1:
                    put(array, across, across, False)
                if number == 3:
                    put(array, across, left, True)
            put(array, ring % 2, ring % 2 + 2, True)

        def compose(before):
            inner = product3(t_high[...], t_low[...], a_high[...], a_low[...])
            return before + times_full(inner)

        gather_own(0, (2, 3))
        hand_own(0)
        wait_beside(0)
        gather_own(0, (0, 1))
        gather_near(0)
        hand_own(1)
        wait_beside(1)
        gather_own(1, (2, 3, 0, 1))

        @pl.when(row == last)
        def _():
            wait_beside(2)

            @pl.when(ring >= 2)
            def _():
                shared = full[b_array, rows_of(ring, block), rows_of(ring - 2, block)]
                full[b_array, rows_of(2 * (ring - 2) + 1, chunk), rows_of(ring, block)] = (
                    shared.T[chunk:]
                )

            sum_own(levels + 1, b_array, lambda number: None)

        know(0)
        gather_far(0)
        know(1)
        split_full(0)
        split_turned(0)
        sums[0] = product3(t_high[...], t_low[...], m_high[...], m_low[...])

        @pl.when(row < last)
        def _():
            pass_sum(0)

        gather_near(1)

        @pl.when(row == last)
        def _():
            sum_near(levels + 1, b_array)

        know(2)
        gather_far(1)
        for round in range(3, levels - 1):
            know(round)
        for place in range(4):
            weight_rows(place)
        split_full(1)
        split_turned(1)

        @pl.when(row == last)
        def _():
            sum_far(levels + 1, b_array)
            sums[0] = compose(sums[0])
            pass_sum(0)

        for stage in range(1, levels + 1):
            step = 2 ** (stage - 1)
            array = maps_end + stage

            @pl.when(row + step < rows_total)
            def _(stage=stage, step=step, array=array):
                def arrival(number):
                    wait_for(piece_of(array, ring, number), entry_sem.at[stage, number])

                sum_own(stage, array, arrival)
                sum_near(stage, array)
                if stage > 1:
                    wait_for(full.at[stage], map_sem.at[stage - 1])
                    split_full(stage)
                    split_turned(stage)
                sum_far(stage, array)
                sums[stage] = compose(sums[stage - 1])

            @pl.when(row + step >= rows_total)
            def _(stage=stage):
                sums[stage] = sums[stage - 1]
                wait_passed(stage - 1)

            if stage < levels:
                pass_sum(stage)

        upper = copy(
            sums.at[levels, pl.ds(0, chunk)], o_ref.at[0],
            send_sem.at[0, 0], misc_sem.at[0], partner,
        )
        lower = pltpu.make_async_copy(
            sums.at[levels, pl.ds(chunk, chunk)], o_ref.at[0], misc_sem.at[1]
        )
        upper.start()
        lower.start()

        for stage in range(levels):
            @pl.when(row + 2**stage < rows_total)
            def _(stage=stage):
                wait_passed(stage)

        for stage in range(1, levels + 1):
            @pl.when(row + 2 ** (stage - 1) < rows_total)
            def _(stage=stage):
                wait_sent(send_sem.at[stage, 0], 1, 15 * piece // 2)

        @pl.when(row == last)
        def _():
            wait_sent(send_sem.at[levels + 1, 2], 1, 15 * piece // 2)

        for kind in range(2):
            wait_sent(send_sem.at[levels + 1 + kind, 0], 2, 12 * piece)
        lower.wait()
        upper.wait_send()

    for kind in range(2):
        wait_sent(send_sem.at[levels + 1 + kind, 1], 1, chunk)

    @pl.when((row == last) & (core == 0))
    def _():
        wait_sent(send_sem.at[levels + 3, 1], 1, chunk)


def on_device(rows_total, diag_tiles, sub_tiles, boundary):
    size = diag_tiles.shape[-1]
    levels = rows_total.bit_length() - 1
    block = size // 4
    arrays = 2 * levels + 3
    return pl.pallas_call(
        functools.partial(kernel, rows_total, levels),
        out_shape=jax.ShapeDtypeStruct(diag_tiles.shape, F32),
        in_specs=[pl.BlockSpec(memory_space=pl.ANY)] * 3,
        out_specs=pl.BlockSpec(memory_space=pl.ANY),
        scratch_shapes=[
            pltpu.VMEM((arrays, size, size), F32),
            pltpu.VMEM((levels + 1, block, size), F32),
            pltpu.VMEM((levels, size // 8, block), F32),
            pltpu.VMEM((size, size), BF16),
            pltpu.VMEM((size, size), BF16),
            pltpu.VMEM((block, size), BF16),
            pltpu.VMEM((block, size), BF16),
            pltpu.VMEM((size, size), BF16),
            pltpu.VMEM((size, size), BF16),
            pltpu.SemaphoreType.DMA((3, 14)),
            pltpu.SemaphoreType.DMA((2, 24)),
            pltpu.SemaphoreType.DMA((levels + 1, 5)),
            pltpu.SemaphoreType.DMA((levels,)),
            pltpu.SemaphoreType.DMA((4,)),
            pltpu.SemaphoreType.DMA((levels + 4, 3)),
            pltpu.SemaphoreType.REGULAR((levels - 1,)),
        ],
        compiler_params=pltpu.CompilerParams(
            collective_id=0, has_side_effects=True, vmem_limit_bytes=60 * 1024 * 1024
        ),
    )(diag_tiles, sub_tiles, boundary)


def solution(mesh):
    spec = jax.sharding.PartitionSpec
    tiles = spec("row", "col", None)
    return jax.shard_map(
        functools.partial(on_device, mesh.shape["row"]),
        mesh=mesh,
        in_specs=(tiles, tiles, spec("col", None)),
        out_specs=tiles,
        check_vma=False,
    )
```

```python
import functools

import jax
import jax.numpy as jnp
from jax import lax
from jax.experimental import pallas as pl
from jax.experimental.pallas import tpu as pltpu

MESH = pl.DeviceIdType.MESH
BF16 = jnp.bfloat16
F32 = jnp.float32


def split(value):
    high = value.astype(BF16)
    low = (value - high.astype(F32)).astype(BF16)
    return high, low


def dot(left, right):
    return jnp.dot(left, right, preferred_element_type=F32)


def product3(left_high, left_low, right_high, right_low):
    rows = left_high.shape[0]
    both = dot(jnp.concatenate([left_high, left_low], axis=0), right_high)
    return both[:rows] + both[rows:] + dot(left_high, right_low)


def kernel(
    rows_total, levels, d_ref, s_ref, b_ref, o_ref,
    full, sums, halves, m_high, m_low, t_high, t_low, a_high, a_low,
    input_sem, ring_sem, entry_sem, map_sem, misc_sem, send_sem, known_sem,
):
    maps_end = levels
    s_array = 2 * levels + 1
    b_array = 2 * levels + 2
    size = d_ref.shape[-1]
    chunk = size // 8
    block = size // 4
    piece = size // 16
    row = lax.axis_index("row")
    col = lax.axis_index("col")
    ring = col // 2
    core = col % 2
    right = (ring + 1) % 4
    left = (ring + 3) % 4
    across = (ring + 2) % 4
    partner = (row, 2 * ring + (1 - core))
    to_right = (row, 2 * right + core)
    to_left = (row, 2 * left + core)
    last = rows_total - 1

    def rows_of(number, length):
        return pl.ds(pl.multiple_of(number * length, length), length)

    def copy(src, dst, send, recv, device):
        return pltpu.make_async_remote_copy(
            src_ref=src, dst_ref=dst, send_sem=send, recv_sem=recv,
            device_id=device, device_id_type=MESH,
        )

    def wait_for(ref, sem):
        copy(ref, ref, send_sem.at[0, 0], sem, partner).wait_recv()

    def wait_sent(sem, arrays, rows):
        some = full.at[pl.ds(0, arrays), pl.ds(0, rows)]
        copy(some, some, sem, misc_sem.at[0], partner).wait_send()

    mine = 2 * ring + core
    own_rows = rows_of(mine, chunk)
    inputs = ((d_ref.at[0], 0), (s_ref.at[0], s_array), (b_ref, b_array))
    fetches = [
        pltpu.make_async_copy(ref, full.at[array, own_rows], misc_sem.at[1 + k])
        for k, (ref, array) in enumerate(inputs)
    ]
    for fetch in fetches:
        fetch.start()

    def rows_away(step):
        return ((row + step) % rows_total, col), ((row + rows_total - step) % rows_total, col)

    def tell(round):
        for device in rows_away(2**round):
            pl.semaphore_signal(
                known_sem.at[round], inc=1, device_id=device, device_id_type=MESH
            )

    def know(round):
        pl.semaphore_wait(known_sem.at[round], 2)
        if round < levels - 2:
            tell(round + 1)

    barrier = pltpu.get_barrier_semaphore()
    greeted = (partner, to_right, to_left, *rows_away(1))
    for device in greeted:
        pl.semaphore_signal(barrier, inc=1, device_id=device, device_id_type=MESH)
    for fetch in fetches:
        fetch.wait()
    pl.semaphore_wait(barrier, len(greeted))
    tell(0)

    def near_link_last(from_left, from_right):
        @pl.when(ring < 2)
        def _():
            from_right()
            from_left()

        @pl.when(ring >= 2)
        def _():
            from_left()
            from_right()

    def input_piece(kind, place, number):
        return full.at[inputs[kind][1], rows_of(4 * place + number, piece)]

    def send_input(kind, place, number, device, slot):
        here = input_piece(kind, place, number)
        copy(here, here, send_sem.at[levels + 1 + kind, 0], input_sem.at[kind, slot], device).start()

    def wait_input(kind, place, number, slot):
        wait_for(input_piece(kind, place, number), input_sem.at[kind, slot])

    def hand_own(kind):
        here = full.at[inputs[kind][1], own_rows]
        copy(here, here, send_sem.at[levels + 1 + kind, 1], input_sem.at[kind, 12], partner).start()

    def gather_own(kind, numbers):
        for number in numbers:
            send_input(kind, ring, number, to_right, number)
        for number in reversed(numbers):
            send_input(kind, ring, number, to_left, 4 + number)

    def gather_near(kind):
        def from_left():
            for number in (2, 0, 3, 1):
                wait_input(kind, left, number, number)
                if number % 2 == 0:
                    send_input(kind, left, number, to_right, 8 + number)
                send_input(kind, left, number, partner, 13)

        def from_right():
            for number in (3, 1, 2, 0):
                wait_input(kind, right, number, 4 + number)
                if number % 2 == 1:
                    send_input(kind, right, number, to_left, 8 + number)
                send_input(kind, right, number, partner, 13)

        near_link_last(from_left, from_right)

    def gather_far(kind):
        for number in (2, 3, 0, 1):
            wait_input(kind, across, number, 8 + number)
            send_input(kind, across, number, partner, 13)

    def wait_beside(kind):
        wait_for(full.at[0, pl.ds(0, chunk)], input_sem.at[kind, 12])

    def wait_others(kind):
        wait_for(full.at[0, pl.ds(0, 3 * block)], input_sem.at[kind, 13])

    def split_full(array):
        for place in range(4):
            rows = pl.ds(place * block, block)
            m_high[rows], m_low[rows] = split(full[array, rows])

    def split_turned(array):
        t_high[...], t_low[...] = split(full[array, :, rows_of(ring, block)].T)

    def times_full(value):
        high, low = split(value)
        return product3(high, low, m_high[...], m_low[...])

    def weight_rows(place):
        rows = rows_of(place, block)
        full[1, rows] = times_full(full[s_array, rows])

    @pl.when(core == 0)
    def _():
        hand_own(0)
        hand_own(1)

        @pl.when(row == last)
        def _():
            hand_own(2)

        def quarter_of(array, place, quarter):
            return full.at[array, rows_of(4 * place + quarter, piece)]

        def pass_map(stage):
            @pl.when(row >= 2**stage)
            def _():
                for quarter in range(4):
                    copy(
                        quarter_of(stage + 1, ring, quarter),
                        quarter_of(maps_end + stage + 1, ring, quarter),
                        send_sem.at[stage, 1], entry_sem.at[stage + 1, quarter],
                        (row - 2**stage, col),
                    ).start()

        wait_beside(0)
        know(0)
        wait_beside(1)
        know(1)
        wait_others(0)

        @pl.when(row < last)
        def _():
            split_full(0)
            weight_rows(ring)
            pass_map(0)

        for round in range(2, levels - 1):
            know(round)
        wait_others(1)

        @pl.when(row < last)
        def _():
            for place in (left, right, across):
                weight_rows(place)

        for stage in range(1, levels):
            @pl.when(row + 2**stage < rows_total)
            def _(stage=stage):
                array = stage + 1

                def eighth_of(place, eighth):
                    return full.at[array, rows_of(8 * place + eighth, piece // 2)]

                def send(place, eighth, device, slot):
                    here = eighth_of(place, eighth)
                    copy(
                        here, here, send_sem.at[stage, 0], ring_sem.at[stage % 2, slot], device
                    ).start()

                def hand_over(place, eighth):
                    here = eighth_of(place, eighth)
                    copy(here, here, send_sem.at[stage, 2], map_sem.at[stage], partner).start()

                def wait(place, eighth, slot):
                    wait_for(eighth_of(place, eighth), ring_sem.at[stage % 2, slot])

                split_full(stage)
                for quarter in range(4):
                    wait_for(
                        quarter_of(maps_end + stage, ring, quarter), entry_sem.at[stage, quarter]
                    )
                rows = rows_of(ring, block)
                full[array, rows] = times_full(full[maps_end + stage, rows])
                for eighth in (0, 2, 4, 6, 1, 3, 5, 7):
                    other = eighth + 1 - 2 * (eighth % 2)
                    send(ring, eighth, to_right, eighth)
                    send(ring, other, to_left, 8 + other)
                if stage < levels - 1:
                    pass_map(stage)
                for eighth in range(8):
                    hand_over(ring, eighth)

                def from_left():
                    for eighth in (0, 2, 4, 6):
                        wait(left, eighth, eighth)
                        send(left, eighth, to_right, 16 + eighth)
                        hand_over(left, eighth)

                def from_right():
                    for eighth in (1, 3, 5, 7):
                        wait(right, eighth, 8 + eighth)
                        send(right, eighth, to_left, 16 + eighth)
                        hand_over(right, eighth)

                near_link_last(from_left, from_right)
                for eighth in (0, 2, 4, 6):
                    wait(left, eighth + 1, eighth + 1)
                    hand_over(left, eighth + 1)
                    wait(right, eighth, 8 + eighth)
                    hand_over(right, eighth)
                for eighth in range(8):
                    wait(across, eighth, 16 + eighth)
                    hand_over(across, eighth)

        @pl.when((row < last) & (row >= 1))
        def _():
            wait_sent(send_sem.at[0, 1], 1, block)

        for stage in range(1, levels):
            @pl.when(row + 2**stage < rows_total)
            def _(stage=stage):
                wait_sent(send_sem.at[stage, 0], 3, block)
                wait_sent(send_sem.at[stage, 2], 1, size)
                if stage < levels - 1:
                    @pl.when(row >= 2**stage)
                    def _():
                        wait_sent(send_sem.at[stage, 1], 1, block)

        wait_for(o_ref.at[0], misc_sem.at[0])

    @pl.when(core == 1)
    def _():
        def piece_of(array, place, number):
            if number < 4:
                first, second = 2 * place + number % 2, (place + number // 2) % 4
            else:
                first, second = 2 * (place % 2) + place // 2, place % 2 + 2
            return full.at[array, rows_of(first, chunk), rows_of(second, block)]

        def pass_sum(stage):
            target = maps_end + stage + 1

            @pl.when(row >= 2**stage)
            def _():
                def start(source, number):
                    copy(
                        source, piece_of(target, ring, number),
                        send_sem.at[stage, 1], entry_sem.at[stage + 1, number],
                        (row - 2**stage, col),
                    ).start()

                for number in range(4):
                    start(
                        sums.at[
                            stage, pl.ds(number % 2 * chunk, chunk),
                            rows_of((ring + number // 2) % 4, block),
                        ],
                        number,
                    )
                shared = sums[stage, :, rows_of(across, block)]

                @pl.when(ring < 2)
                def _():
                    halves[stage] = shared[:chunk]

                @pl.when(ring >= 2)
                def _():
                    halves[stage] = shared.T[chunk:]

                start(halves.at[stage], 4)

        def wait_passed(stage):
            @pl.when(row >= 2**stage)
            def _():
                wait_sent(send_sem.at[stage, 1], 1, 5 * piece // 2)

        def put(array, place, second, turn):
            rows, columns = rows_of(place, block), rows_of(second, block)
            value = full[array, rows, columns]
            a_high[rows, columns], a_low[rows, columns] = split(value)
            if turn:
                a_high[columns, rows], a_low[columns, rows] = split(value.T)

        def send_sum(stage, array, place, number, device, slot):
            here = piece_of(array, place, number)
            sent = send_sem.at[stage, 0] if stage <= levels else send_sem.at[levels + 1, 2]
            copy(here, here, sent, ring_sem.at[stage % 2, slot + number], device).start()

        def wait_sum(stage, array, place, number, slot):
            wait_for(piece_of(array, place, number), ring_sem.at[stage % 2, slot + number])

        def sum_own(stage, array, arrival):
            for number in range(5):
                arrival(number)
                send_sum(stage, array, ring, number, to_right, 0)
                send_sum(stage, array, ring, number, to_left, 5)
            put(array, ring, ring, False)
            put(array, ring, right, True)

        def sum_near(stage, array):
            def from_left():
                for number in (0, 2, 4):
                    wait_sum(stage, array, left, number, 0)
                    send_sum(stage, array, left, number, to_right, 10)

            def from_right():
                for number in (1, 3):
                    wait_sum(stage, array, right, number, 5)
                    send_sum(stage, array, right, number, to_left, 10)

            near_link_last(from_left, from_right)
            wait_sum(stage, array, left, 1, 0)
            put(array, left, left, False)
            wait_sum(stage, array, right, 0, 5)
            put(array, right, right, False)
            wait_sum(stage, array, left, 3, 0)
            put(array, left, ring, True)
            wait_sum(stage, array, right, 2, 5)
            put(array, right, across, True)
            wait_sum(stage, array, right, 4, 5)
            put(array, left % 2, left % 2 + 2, True)

        def sum_far(stage, array):
            for number in range(5):
                wait_sum(stage, array, across, number, 10)
                if number == 1:
                    put(array, across, across, False)
                if number == 3:
                    put(array, across, left, True)
            put(array, ring % 2, ring % 2 + 2, True)

        def compose(before):
            inner = product3(t_high[...], t_low[...], a_high[...], a_low[...])
            return before + times_full(inner)

        gather_own(0, (2, 3))
        hand_own(0)
        wait_beside(0)
        gather_own(0, (0, 1))
        gather_near(0)
        hand_own(1)
        wait_beside(1)
        gather_own(1, (2, 3, 0, 1))

        @pl.when(row == last)
        def _():
            wait_beside(2)

            @pl.when(ring >= 2)
            def _():
                shared = full[b_array, rows_of(ring, block), rows_of(ring - 2, block)]
                full[b_array, rows_of(2 * (ring - 2) + 1, chunk), rows_of(ring, block)] = (
                    shared.T[chunk:]
                )

            sum_own(levels + 1, b_array, lambda number: None)

        know(0)
        gather_far(0)
        know(1)
        split_full(0)
        split_turned(0)
        sums[0] = product3(t_high[...], t_low[...], m_high[...], m_low[...])

        @pl.when(row < last)
        def _():
            pass_sum(0)

        gather_near(1)

        @pl.when(row == last)
        def _():
            sum_near(levels + 1, b_array)

        know(2)
        gather_far(1)
        for round in range(3, levels - 1):
            know(round)
        for place in range(4):
            weight_rows(place)
        split_full(1)
        split_turned(1)

        @pl.when(row == last)
        def _():
            sum_far(levels + 1, b_array)
            sums[0] = compose(sums[0])
            pass_sum(0)

        for stage in range(1, levels + 1):
            step = 2 ** (stage - 1)
            array = maps_end + stage

            @pl.when(row + step < rows_total)
            def _(stage=stage, step=step, array=array):
                def arrival(number):
                    wait_for(piece_of(array, ring, number), entry_sem.at[stage, number])

                sum_own(stage, array, arrival)
                sum_near(stage, array)
                if stage > 1:
                    wait_for(full.at[stage], map_sem.at[stage - 1])
                    split_full(stage)
                    split_turned(stage)
                sum_far(stage, array)
                sums[stage] = compose(sums[stage - 1])

            @pl.when(row + step >= rows_total)
            def _(stage=stage):
                sums[stage] = sums[stage - 1]
                wait_passed(stage - 1)

            if stage < levels:
                pass_sum(stage)

        upper = copy(
            sums.at[levels, pl.ds(0, chunk)], o_ref.at[0],
            send_sem.at[0, 0], misc_sem.at[0], partner,
        )
        upper.start()
        o_ref[0] = sums[levels, pl.ds(chunk, chunk)]

        for stage in range(levels):
            @pl.when(row + 2**stage < rows_total)
            def _(stage=stage):
                wait_passed(stage)

        for stage in range(1, levels + 1):
            @pl.when(row + 2 ** (stage - 1) < rows_total)
            def _(stage=stage):
                wait_sent(send_sem.at[stage, 0], 1, 15 * piece // 2)

        @pl.when(row == last)
        def _():
            wait_sent(send_sem.at[levels + 1, 2], 1, 15 * piece // 2)

        for kind in range(2):
            wait_sent(send_sem.at[levels + 1 + kind, 0], 2, 12 * piece)
        upper.wait_send()

    for kind in range(2):
        wait_sent(send_sem.at[levels + 1 + kind, 1], 1, chunk)

    @pl.when((row == last) & (core == 0))
    def _():
        wait_sent(send_sem.at[levels + 3, 1], 1, chunk)


def on_device(rows_total, diag_tiles, sub_tiles, boundary):
    size = diag_tiles.shape[-1]
    levels = rows_total.bit_length() - 1
    block = size // 4
    arrays = 2 * levels + 3
    return pl.pallas_call(
        functools.partial(kernel, rows_total, levels),
        out_shape=jax.ShapeDtypeStruct(diag_tiles.shape, F32),
        in_specs=[pl.BlockSpec(memory_space=pl.ANY)] * 3,
        out_specs=pl.BlockSpec(memory_space=pltpu.VMEM),
        scratch_shapes=[
            pltpu.VMEM((arrays, size, size), F32),
            pltpu.VMEM((levels + 1, block, size), F32),
            pltpu.VMEM((levels, size // 8, block), F32),
            pltpu.VMEM((size, size), BF16),
            pltpu.VMEM((size, size), BF16),
            pltpu.VMEM((block, size), BF16),
            pltpu.VMEM((block, size), BF16),
            pltpu.VMEM((size, size), BF16),
            pltpu.VMEM((size, size), BF16),
            pltpu.SemaphoreType.DMA((3, 14)),
            pltpu.SemaphoreType.DMA((2, 24)),
            pltpu.SemaphoreType.DMA((levels + 1, 5)),
            pltpu.SemaphoreType.DMA((levels,)),
            pltpu.SemaphoreType.DMA((4,)),
            pltpu.SemaphoreType.DMA((levels + 4, 3)),
            pltpu.SemaphoreType.REGULAR((levels - 1,)),
        ],
        compiler_params=pltpu.CompilerParams(
            collective_id=0, has_side_effects=True, vmem_limit_bytes=55040 * 1024
        ),
    )(diag_tiles, sub_tiles, boundary)


def solution(mesh):
    spec = jax.sharding.PartitionSpec
    tiles = spec("row", "col", None)
    return jax.shard_map(
        functools.partial(on_device, mesh.shape["row"]),
        mesh=mesh,
        in_specs=(tiles, tiles, spec("col", None)),
        out_specs=tiles,
        check_vma=False,
    )
```

```python
import functools

import jax
import jax.numpy as jnp
from jax import lax
from jax.experimental import pallas as pl
from jax.experimental.pallas import tpu as pltpu

MESH = pl.DeviceIdType.MESH
BF16 = jnp.bfloat16
F32 = jnp.float32


def split(value):
    high = value.astype(BF16)
    low = (value - high.astype(F32)).astype(BF16)
    return high, low


def dot(left, right):
    return jnp.dot(left, right, preferred_element_type=F32)


def product3(left_high, left_low, right_high, right_low):
    rows = left_high.shape[0]
    both = dot(jnp.concatenate([left_high, left_low], axis=0), right_high)
    return both[:rows] + both[rows:] + dot(left_high, right_low)


def kernel(
    rows_total, levels, d_ref, s_ref, b_ref, o_ref,
    full, sums, halves, m_high, m_low, t_high, t_low, a_high, a_low,
    input_sem, ring_sem, entry_sem, map_sem, misc_sem, send_sem, known_sem,
):
    maps_end = levels
    s_array = 2 * levels + 1
    b_array = 2 * levels + 2
    size = d_ref.shape[-1]
    chunk = size // 8
    block = size // 4
    piece = size // 16
    row = lax.axis_index("row")
    col = lax.axis_index("col")
    ring = col // 2
    core = col % 2
    right = (ring + 1) % 4
    left = (ring + 3) % 4
    across = (ring + 2) % 4
    partner = (row, 2 * ring + (1 - core))
    to_right = (row, 2 * right + core)
    to_left = (row, 2 * left + core)
    last = rows_total - 1

    def rows_of(number, length):
        return pl.ds(pl.multiple_of(number * length, length), length)

    def copy(src, dst, send, recv, device):
        return pltpu.make_async_remote_copy(
            src_ref=src, dst_ref=dst, send_sem=send, recv_sem=recv,
            device_id=device, device_id_type=MESH,
        )

    def wait_for(ref, sem):
        copy(ref, ref, send_sem.at[0, 0], sem, partner).wait_recv()

    def wait_sent(sem, arrays, rows):
        some = full.at[pl.ds(0, arrays), pl.ds(0, rows)]
        copy(some, some, sem, misc_sem.at[0], partner).wait_send()

    mine = 2 * ring + core
    own_rows = rows_of(mine, chunk)
    inputs = ((d_ref.at[0], 0), (s_ref.at[0], s_array), (b_ref, b_array))
    fetches = [
        pltpu.make_async_copy(ref, full.at[array, own_rows], misc_sem.at[1 + k])
        for k, (ref, array) in enumerate(inputs)
    ]
    for fetch in fetches:
        fetch.start()

    def rows_away(step):
        return ((row + step) % rows_total, col), ((row + rows_total - step) % rows_total, col)

    def tell(round):
        for device in rows_away(2**round):
            pl.semaphore_signal(
                known_sem.at[round], inc=1, device_id=device, device_id_type=MESH
            )

    def know(round):
        pl.semaphore_wait(known_sem.at[round], 2)
        if round < levels - 2:
            tell(round + 1)

    barrier = pltpu.get_barrier_semaphore()
    greeted = (partner, to_right, to_left, *rows_away(1))
    for device in greeted:
        pl.semaphore_signal(barrier, inc=1, device_id=device, device_id_type=MESH)
    for fetch in fetches:
        fetch.wait()
    pl.semaphore_wait(barrier, len(greeted))
    tell(0)

    def near_link_last(from_left, from_right):
        @pl.when(ring < 2)
        def _():
            from_right()
            from_left()

        @pl.when(ring >= 2)
        def _():
            from_left()
            from_right()

    def input_piece(kind, place, number):
        return full.at[inputs[kind][1], rows_of(4 * place + number, piece)]

    def send_input(kind, place, number, device, slot):
        here = input_piece(kind, place, number)
        copy(here, here, send_sem.at[levels + 1 + kind, 0], input_sem.at[kind, slot], device).start()

    def wait_input(kind, place, number, slot):
        wait_for(input_piece(kind, place, number), input_sem.at[kind, slot])

    def hand_own(kind):
        here = full.at[inputs[kind][1], own_rows]
        copy(here, here, send_sem.at[levels + 1 + kind, 1], input_sem.at[kind, 12], partner).start()

    def gather_own(kind, numbers):
        for number in numbers:
            send_input(kind, ring, number, to_right, number)
        for number in reversed(numbers):
            send_input(kind, ring, number, to_left, 4 + number)

    def gather_near(kind):
        def from_left():
            for number in (2, 0, 3, 1):
                wait_input(kind, left, number, number)
                if number % 2 == 0:
                    send_input(kind, left, number, to_right, 8 + number)
                send_input(kind, left, number, partner, 13)

        def from_right():
            for number in (3, 1, 2, 0):
                wait_input(kind, right, number, 4 + number)
                if number % 2 == 1:
                    send_input(kind, right, number, to_left, 8 + number)
                send_input(kind, right, number, partner, 13)

        near_link_last(from_left, from_right)

    def gather_far(kind):
        for number in (2, 3, 0, 1):
            wait_input(kind, across, number, 8 + number)
            send_input(kind, across, number, partner, 13)

    def wait_beside(kind):
        wait_for(full.at[0, pl.ds(0, chunk)], input_sem.at[kind, 12])

    def wait_others(kind):
        wait_for(full.at[0, pl.ds(0, 3 * block)], input_sem.at[kind, 13])

    def split_full(array):
        for place in range(4):
            rows = pl.ds(place * block, block)
            m_high[rows], m_low[rows] = split(full[array, rows])

    def split_turned(array):
        t_high[...], t_low[...] = split(full[array, :, rows_of(ring, block)].T)

    def times_full(value):
        high, low = split(value)
        return product3(high, low, m_high[...], m_low[...])

    def weight_rows(place):
        rows = rows_of(place, block)
        full[1, rows] = times_full(full[s_array, rows])

    @pl.when(core == 0)
    def _():
        hand_own(0)
        hand_own(1)

        @pl.when(row == last)
        def _():
            hand_own(2)

        def quarter_of(array, place, quarter):
            return full.at[array, rows_of(4 * place + quarter, piece)]

        def pass_map(stage):
            @pl.when(row >= 2**stage)
            def _():
                for quarter in range(4):
                    copy(
                        quarter_of(stage + 1, ring, quarter),
                        quarter_of(maps_end + stage + 1, ring, quarter),
                        send_sem.at[stage, 1], entry_sem.at[stage + 1, quarter],
                        (row - 2**stage, col),
                    ).start()

        wait_beside(0)
        know(0)
        wait_beside(1)
        know(1)
        wait_others(0)

        @pl.when(row < last)
        def _():
            split_full(0)
            weight_rows(ring)
            pass_map(0)

        for round in range(2, levels - 1):
            know(round)
        wait_others(1)

        @pl.when(row < last)
        def _():
            for place in (left, right, across):
                weight_rows(place)

        for stage in range(1, levels):
            @pl.when(row + 2**stage < rows_total)
            def _(stage=stage):
                array = stage + 1

                def eighth_of(place, eighth):
                    return full.at[array, rows_of(8 * place + eighth, piece // 2)]

                def send(place, eighth, device, slot):
                    here = eighth_of(place, eighth)
                    copy(
                        here, here, send_sem.at[stage, 0], ring_sem.at[stage % 2, slot], device
                    ).start()

                def hand_over(place, eighth):
                    here = eighth_of(place, eighth)
                    copy(here, here, send_sem.at[stage, 2], map_sem.at[stage], partner).start()

                def wait(place, eighth, slot):
                    wait_for(eighth_of(place, eighth), ring_sem.at[stage % 2, slot])

                split_full(stage)
                for quarter in range(4):
                    wait_for(
                        quarter_of(maps_end + stage, ring, quarter), entry_sem.at[stage, quarter]
                    )
                rows = rows_of(ring, block)
                full[array, rows] = times_full(full[maps_end + stage, rows])
                if stage < levels - 1:
                    pass_map(stage)
                for eighth in (0, 2, 4, 6, 1, 3, 5, 7):
                    other = eighth + 1 - 2 * (eighth % 2)
                    send(ring, eighth, to_right, eighth)
                    send(ring, other, to_left, 8 + other)
                for eighth in range(8):
                    hand_over(ring, eighth)

                def from_left():
                    for eighth in (0, 2, 4, 6):
                        wait(left, eighth, eighth)
                        send(left, eighth, to_right, 16 + eighth)
                        hand_over(left, eighth)

                def from_right():
                    for eighth in (1, 3, 5, 7):
                        wait(right, eighth, 8 + eighth)
                        send(right, eighth, to_left, 16 + eighth)
                        hand_over(right, eighth)

                near_link_last(from_left, from_right)
                for eighth in (0, 2, 4, 6):
                    wait(left, eighth + 1, eighth + 1)
                    hand_over(left, eighth + 1)
                    wait(right, eighth, 8 + eighth)
                    hand_over(right, eighth)
                for eighth in range(8):
                    wait(across, eighth, 16 + eighth)
                    hand_over(across, eighth)

        @pl.when((row < last) & (row >= 1))
        def _():
            wait_sent(send_sem.at[0, 1], 1, block)

        for stage in range(1, levels):
            @pl.when(row + 2**stage < rows_total)
            def _(stage=stage):
                wait_sent(send_sem.at[stage, 0], 3, block)
                wait_sent(send_sem.at[stage, 2], 1, size)
                if stage < levels - 1:
                    @pl.when(row >= 2**stage)
                    def _():
                        wait_sent(send_sem.at[stage, 1], 1, block)

        wait_for(o_ref.at[0], misc_sem.at[0])

    @pl.when(core == 1)
    def _():
        def piece_of(array, place, number):
            if number < 4:
                first, second = 2 * place + number % 2, (place + number // 2) % 4
            else:
                first, second = 2 * (place % 2) + place // 2, place % 2 + 2
            return full.at[array, rows_of(first, chunk), rows_of(second, block)]

        def pass_sum(stage):
            target = maps_end + stage + 1

            @pl.when(row >= 2**stage)
            def _():
                def start(source, number):
                    copy(
                        source, piece_of(target, ring, number),
                        send_sem.at[stage, 1], entry_sem.at[stage + 1, number],
                        (row - 2**stage, col),
                    ).start()

                for number in range(4):
                    start(
                        sums.at[
                            stage, pl.ds(number % 2 * chunk, chunk),
                            rows_of((ring + number // 2) % 4, block),
                        ],
                        number,
                    )
                shared = sums[stage, :, rows_of(across, block)]

                @pl.when(ring < 2)
                def _():
                    halves[stage] = shared[:chunk]

                @pl.when(ring >= 2)
                def _():
                    halves[stage] = shared.T[chunk:]

                start(halves.at[stage], 4)

        def wait_passed(stage):
            @pl.when(row >= 2**stage)
            def _():
                wait_sent(send_sem.at[stage, 1], 1, 5 * piece // 2)

        def put(array, place, second, turn):
            rows, columns = rows_of(place, block), rows_of(second, block)
            value = full[array, rows, columns]
            a_high[rows, columns], a_low[rows, columns] = split(value)
            if turn:
                a_high[columns, rows], a_low[columns, rows] = split(value.T)

        def send_sum(stage, array, place, number, device, slot):
            here = piece_of(array, place, number)
            sent = send_sem.at[stage, 0] if stage <= levels else send_sem.at[levels + 1, 2]
            copy(here, here, sent, ring_sem.at[stage % 2, slot + number], device).start()

        def wait_sum(stage, array, place, number, slot):
            wait_for(piece_of(array, place, number), ring_sem.at[stage % 2, slot + number])

        def sum_own(stage, array, arrival):
            for number in range(5):
                arrival(number)
                send_sum(stage, array, ring, number, to_right, 0)
                send_sum(stage, array, ring, number, to_left, 5)
            put(array, ring, ring, False)
            put(array, ring, right, True)

        def sum_near(stage, array):
            def from_left():
                for number in (0, 2, 4):
                    wait_sum(stage, array, left, number, 0)
                    send_sum(stage, array, left, number, to_right, 10)

            def from_right():
                for number in (1, 3):
                    wait_sum(stage, array, right, number, 5)
                    send_sum(stage, array, right, number, to_left, 10)

            near_link_last(from_left, from_right)
            wait_sum(stage, array, left, 1, 0)
            put(array, left, left, False)
            wait_sum(stage, array, right, 0, 5)
            put(array, right, right, False)
            wait_sum(stage, array, left, 3, 0)
            put(array, left, ring, True)
            wait_sum(stage, array, right, 2, 5)
            put(array, right, across, True)
            wait_sum(stage, array, right, 4, 5)
            put(array, left % 2, left % 2 + 2, True)

        def sum_far(stage, array):
            for number in range(5):
                wait_sum(stage, array, across, number, 10)
                if number == 1:
                    put(array, across, across, False)
                if number == 3:
                    put(array, across, left, True)
            put(array, ring % 2, ring % 2 + 2, True)

        def compose(before):
            inner = product3(t_high[...], t_low[...], a_high[...], a_low[...])
            return before + times_full(inner)

        gather_own(0, (2, 3))
        hand_own(0)
        wait_beside(0)
        gather_own(0, (0, 1))
        gather_near(0)
        hand_own(1)
        wait_beside(1)
        gather_own(1, (2, 3, 0, 1))

        @pl.when(row == last)
        def _():
            wait_beside(2)

            @pl.when(ring >= 2)
            def _():
                shared = full[b_array, rows_of(ring, block), rows_of(ring - 2, block)]
                full[b_array, rows_of(2 * (ring - 2) + 1, chunk), rows_of(ring, block)] = (
                    shared.T[chunk:]
                )

            sum_own(levels + 1, b_array, lambda number: None)

        know(0)
        gather_far(0)
        know(1)
        split_full(0)
        split_turned(0)
        sums[0] = product3(t_high[...], t_low[...], m_high[...], m_low[...])

        @pl.when(row < last)
        def _():
            pass_sum(0)

        gather_near(1)

        @pl.when(row == last)
        def _():
            sum_near(levels + 1, b_array)

        know(2)
        gather_far(1)
        for round in range(3, levels - 1):
            know(round)
        for place in range(4):
            weight_rows(place)
        split_full(1)
        split_turned(1)

        @pl.when(row == last)
        def _():
            sum_far(levels + 1, b_array)
            sums[0] = compose(sums[0])
            pass_sum(0)

        for stage in range(1, levels + 1):
            step = 2 ** (stage - 1)
            array = maps_end + stage

            @pl.when(row + step < rows_total)
            def _(stage=stage, step=step, array=array):
                def arrival(number):
                    wait_for(piece_of(array, ring, number), entry_sem.at[stage, number])

                sum_own(stage, array, arrival)
                sum_near(stage, array)
                if stage > 1:
                    wait_for(full.at[stage], map_sem.at[stage - 1])
                    split_full(stage)
                    split_turned(stage)
                sum_far(stage, array)
                sums[stage] = compose(sums[stage - 1])

            @pl.when(row + step >= rows_total)
            def _(stage=stage):
                sums[stage] = sums[stage - 1]
                wait_passed(stage - 1)

            if stage < levels:
                pass_sum(stage)

        upper = copy(
            sums.at[levels, pl.ds(0, chunk)], o_ref.at[0],
            send_sem.at[0, 0], misc_sem.at[0], partner,
        )
        upper.start()
        o_ref[0] = sums[levels, pl.ds(chunk, chunk)]

        for stage in range(levels):
            @pl.when(row + 2**stage < rows_total)
            def _(stage=stage):
                wait_passed(stage)

        for stage in range(1, levels + 1):
            @pl.when(row + 2 ** (stage - 1) < rows_total)
            def _(stage=stage):
                wait_sent(send_sem.at[stage, 0], 1, 15 * piece // 2)

        @pl.when(row == last)
        def _():
            wait_sent(send_sem.at[levels + 1, 2], 1, 15 * piece // 2)

        for kind in range(2):
            wait_sent(send_sem.at[levels + 1 + kind, 0], 2, 12 * piece)
        upper.wait_send()

    for kind in range(2):
        wait_sent(send_sem.at[levels + 1 + kind, 1], 1, chunk)

    @pl.when((row == last) & (core == 0))
    def _():
        wait_sent(send_sem.at[levels + 3, 1], 1, chunk)


def on_device(rows_total, diag_tiles, sub_tiles, boundary):
    size = diag_tiles.shape[-1]
    levels = rows_total.bit_length() - 1
    block = size // 4
    arrays = 2 * levels + 3
    return pl.pallas_call(
        functools.partial(kernel, rows_total, levels),
        out_shape=jax.ShapeDtypeStruct(diag_tiles.shape, F32),
        in_specs=[pl.BlockSpec(memory_space=pl.ANY)] * 3,
        out_specs=pl.BlockSpec(memory_space=pltpu.VMEM),
        scratch_shapes=[
            pltpu.VMEM((arrays, size, size), F32),
            pltpu.VMEM((levels + 1, block, size), F32),
            pltpu.VMEM((levels, size // 8, block), F32),
            pltpu.VMEM((size, size), BF16),
            pltpu.VMEM((size, size), BF16),
            pltpu.VMEM((block, size), BF16),
            pltpu.VMEM((block, size), BF16),
            pltpu.VMEM((size, size), BF16),
            pltpu.VMEM((size, size), BF16),
            pltpu.SemaphoreType.DMA((3, 14)),
            pltpu.SemaphoreType.DMA((2, 24)),
            pltpu.SemaphoreType.DMA((levels + 1, 5)),
            pltpu.SemaphoreType.DMA((levels,)),
            pltpu.SemaphoreType.DMA((4,)),
            pltpu.SemaphoreType.DMA((levels + 4, 3)),
            pltpu.SemaphoreType.REGULAR((levels - 1,)),
        ],
        compiler_params=pltpu.CompilerParams(
            collective_id=0, has_side_effects=True, vmem_limit_bytes=55040 * 1024
        ),
    )(diag_tiles, sub_tiles, boundary)


def solution(mesh):
    spec = jax.sharding.PartitionSpec
    tiles = spec("row", "col", None)
    return jax.shard_map(
        functools.partial(on_device, mesh.shape["row"]),
        mesh=mesh,
        in_specs=(tiles, tiles, spec("col", None)),
        out_specs=tiles,
        check_vma=False,
    )
```
